256 devices in a mesh: gx: 16 (over z, x_lo), gz: 16 (over y, x_hi, core).
Axes of the slice: x: 4 (x_hi: 2, x_lo: 2; x = x_hi * 2 + x_lo), y: 4, z: 8, core: 2. Of those that a mesh axis runs over, the one named last changes fastest.
Arguments:
- velocity: float32 [3, 128, 512, 384], P(None, 'gx', 'gz'), may hold values from -6 to 6
- y_gap: float32 [385], replicated, may hold values from 0.2 to 2
Outputs:
- eddy_visc: float32 [128, 512, 384], P('gx', 'gz')
- lm_field: float32 [128, 512, 384], P('gx', 'gz')
- mm_field: float32 [128, 512, 384], P('gx', 'gz')
- coefficient: float32 [384], replicated
The draws below stay inside these ranges and needn't reach their ends.
All inputs are finite; a program needn't handle non-finite values.
Results may differ from the reference program's by a relative error of at most 0.00002.
Values sent between devices are 32-bit elements; how exact they have to be, the bound alone decides.
A program may use at most 64 MiB of HBM per device.

```python
import math
import jax
import jax.numpy as jnp
from jax import lax

NY = 384
NX = 128
NZ = 512


def block_levels(key, shape, split, smallest, top_value):
    gain, own = 1.0, jax.random.fold_in(key, 6)
    for dim, shards_of in split:
        draws = jnp.exp(jax.random.uniform(jax.random.fold_in(own, dim), (shards_of,), jnp.float32, smallest / len(split), top_value / len(split)))
        gain = gain * jnp.repeat(draws, shape[dim] // shards_of).reshape([-1 if axis == dim else 1 for axis in range(len(shape))])
    return gain


def scatter_about(stream_key, extent, spread, bound, cuts=(), held_as=jnp.bfloat16):
    entries = spread * jax.random.normal(stream_key, extent, jnp.float32)
    if cuts:
        entries = entries * block_levels(stream_key, extent, cuts, -0.22, 0.18)
    return jnp.clip(entries, -bound, bound).astype(held_as)


def setup_inputs(seed: int = 0) -> dict:
    arg_keys = jax.random.split(jax.random.key(seed), 3)
    velocity = scatter_about(arg_keys[0], (3, NX, NZ, NY), 1.0, 6.0, ((1, 16), (2, 16)), jnp.float32)
    y_gap = jnp.clip(jnp.exp(jax.random.uniform(arg_keys[1], (NY + 1,), jnp.float32, math.log(0.2), math.log(2.0))), 0.2, 2.0)
    return dict(velocity=velocity, y_gap=y_gap)


WEIGHTS = (1.0, 1.0, 1.0, 2.0, 2.0, 2.0)

def wall_slope(values, y_gap):
    padded = jnp.pad(values, [(0, 0)] * (values.ndim - 1) + [(1, 1)])
    return (padded[..., 2:] - padded[..., :-2]) / (y_gap[:-1] + y_gap[1:])

def strain_parts(slope_x, slope_y, slope_z):
    return jnp.stack([slope_x[0], slope_y[1], slope_z[2], 0.5 * (slope_y[0] + slope_x[1]), 0.5 * (slope_z[0] + slope_x[2]), 0.5 * (slope_z[1] + slope_y[2])])

def contract(first_part, second_part):
    summed = first_part[0] * second_part[0]
    for component in range(1, 6):
        summed = summed + WEIGHTS[component] * first_part[component] * second_part[component]
    return summed

def magnitude(strain):
    return jnp.sqrt(2.0 * contract(strain, strain))

def pair_products(speeds):
    return jnp.stack([speeds[0] * speeds[0], speeds[1] * speeds[1], speeds[2] * speeds[2], speeds[0] * speeds[1], speeds[0] * speeds[2], speeds[1] * speeds[2]])

def width_square(y_gap):
    return (0.5 * (y_gap[:-1] + y_gap[1:])) ** (2.0 / 3.0)

def germano(smooth_velocity, smooth_pairs, smooth_stress, test_strain, width_sq):
    leonard = smooth_pairs - pair_products(smooth_velocity)
    model_term = 2.0 * width_sq * (smooth_stress - 4.0 * magnitude(test_strain) * test_strain)
    return (contract(leonard, model_term), contract(model_term, model_term))

def periodic_strain(speeds, y_gap):
    slope_x = (jnp.roll(speeds, -1, 1) - jnp.roll(speeds, 1, 1)) * 0.5
    slope_z = (jnp.roll(speeds, -1, 2) - jnp.roll(speeds, 1, 2)) * 0.5
    slope_y = wall_slope(speeds, y_gap)
    return strain_parts(slope_x, slope_y, slope_z)

def periodic_filter(values):
    along_x = 0.25 * jnp.roll(values, 1, 1) + 0.5 * values + 0.25 * jnp.roll(values, -1, 1)
    return 0.25 * jnp.roll(along_x, 1, 2) + 0.5 * along_x + 0.25 * jnp.roll(along_x, -1, 2)

def reference(velocity, y_gap):
    width_sq = width_square(y_gap)
    strain = periodic_strain(velocity, y_gap)
    strain_size = magnitude(strain)
    smooth_velocity = periodic_filter(velocity)
    smooth_pairs = periodic_filter(pair_products(velocity))
    smooth_stress = periodic_filter(strain_size * strain)
    test_strain = periodic_strain(smooth_velocity, y_gap)
    lm_field, mm_field = germano(smooth_velocity, smooth_pairs, smooth_stress, test_strain, width_sq)
    planes = NX * NZ
    numerator = lax.optimization_barrier(jnp.sum(lm_field, axis=(0, 1)))
    denominator = lax.optimization_barrier(jnp.sum(mm_field, axis=(0, 1)))
    coefficient = numerator / planes / (denominator / planes + 1e-06)
    eddy_visc = coefficient * width_sq * strain_size
    return (eddy_visc, lm_field, mm_field, coefficient)
```

```python
import jax
import jax.numpy as jnp
from jax import lax
from jax.experimental import pallas as pl
from jax.experimental.pallas import tpu as pltpu
from jax.sharding import Mesh
from jax.sharding import PartitionSpec as P

AXES = ("gx_0", "gx_1", "gz_0", "gz_1", "gz_2")
GX = ("gx_0", "gx_1")
GZ = ("gz_0", "gz_1", "gz_2")
MESH = pl.DeviceIdType.MESH

LANES = 128
ROWS = 8
TINY = 1.1754944e-38
ORDER = (0, 3, 1, 2)


def root(square):
    return square * lax.rsqrt(jnp.maximum(square, TINY))


def kernel(sizes, planes, vel, gaps, eddy, lm_out, mm_out, coef_out, pad, field, acc, sent, plane_in, line_in,
           load_sem, send_sem, recv_sem, plane_send, plane_recv, line_send, line_recv):
    nz, nxl, ny, nxh, nc = sizes
    nx, depth = vel.shape[1], vel.shape[2]
    chunks = vel.shape[3] // LANES
    tiles = depth // ROWS
    me = tuple(lax.axis_index(name) for name in AXES)

    loads = []
    for part in range(3):
        for chunk in range(chunks):
            loads.append(
                pltpu.make_async_copy(
                    vel.at[part, :, :, pl.ds(chunk * LANES, LANES)],
                    pad.at[part, chunk, pl.ds(2, nx), pl.ds(2, depth), :],
                    load_sem.at[part * chunks + chunk],
                )
            )
    for load in loads:
        load.start()

    def along_x(step):
        ring = nz * nxl
        spot = lax.rem(me[0] * nxl + me[1] + step + ring, ring)
        return (spot // nxl, lax.rem(spot, nxl), me[2], me[3], me[4])

    def along_z(step):
        ring = ny * nxh * nc
        spot = lax.rem((me[2] * nxh + me[3]) * nc + me[4] + step + ring, ring)
        return (me[0], me[1], spot // (nxh * nc), lax.rem(spot // nc, nxh), lax.rem(spot, nc))

    plane = [(a, b, c, d) for a in range(nxl) for b in range(ny) for c in range(nxh) for d in range(nc)]

    def in_plane(off, sign):
        step = [lax.rem(m + sign * o + n, n) for m, o, n in zip(me[1:], off, (nxl, ny, nxh, nc))]
        return (me[0], *step)

    def plane_slot(spot):
        return ((spot[1] * ny + spot[2]) * nxh + spot[3]) * nc + spot[4]

    def on_line(off, sign):
        return (lax.rem(me[0] + sign * off + nz, nz), *me[1:])

    barrier = pltpu.get_barrier_semaphore()
    outside = jnp.where(me[1] == nxl - 1, 1, -1)
    greeted = [along_x(outside)] + [in_plane(off, 1) for off in plane[1:]] + [on_line(off, 1) for off in range(1, nz)]
    for other in greeted:
        pl.semaphore_signal(barrier, inc=1, device_id=other, device_id_type=MESH)
    acc[...] = jnp.zeros_like(acc)
    pl.semaphore_wait(barrier, len(greeted))
    for load in loads:
        load.wait()

    def rim(number, source, target, other):
        return pltpu.make_async_remote_copy(
            src_ref=pad.at[:, :, pl.ds(*source[0]), pl.ds(*source[1]), :],
            dst_ref=pad.at[:, :, pl.ds(*target[0]), pl.ds(*target[1]), :],
            send_sem=send_sem.at[number],
            recv_sem=recv_sem.at[number],
            device_id=other,
            device_id_type=MESH,
        )

    up, down, right, left = along_x(1), along_x(-1), along_z(1), along_z(-1)
    body = (2, nx)
    sides = [
        rim(0, (body, (depth, 2)), (body, (0, 2)), right),
        rim(1, (body, (2, 2)), (body, (depth + 2, 2)), left),
    ]
    strips = []
    for tile in range(tiles):
        cut = (2 + ROWS * tile, ROWS)
        strips.append((
            rim(2 + 2 * tile, ((nx, 2), cut), ((0, 2), cut), up),
            rim(3 + 2 * tile, ((2, 2), cut), ((nx + 2, 2), cut), down),
        ))
    first = 2 + 2 * tiles
    ends = [(0, 2), (nx + 2, 2)]
    corners_left = [rim(first + k, (end, (2, 2)), (end, (depth + 2, 2)), left) for k, end in enumerate(ends)]
    corners_right = [rim(first + 2 + k, (end, (depth, 2)), (end, (0, 2)), right) for k, end in enumerate(ends)]

    for side in sides:
        side.start()
    for tile in ORDER:
        for strip in strips[tile]:
            strip.start()

    lane = lax.broadcasted_iota(jnp.int32, (ROWS, LANES), 1)
    low, high = lane == 0, lane == LANES - 1
    zero = jnp.zeros((ROWS, LANES), jnp.float32)

    def strains(row, tile):
        here, at = row + 2, ROWS * tile + 1

        def speed(part, chunk, dx=0, dz=0):
            return pad[part, chunk, here + dx, pl.ds(at + dz, ROWS), :]

        middle = [[speed(part, chunk) for chunk in range(chunks)] for part in range(3)]
        before = [[pltpu.roll(v, 1, 1) for v in parts] for parts in middle]
        after = [[pltpu.roll(v, LANES - 1, 1) for v in parts] for parts in middle]
        for chunk in range(chunks):
            rate = jnp.broadcast_to(gaps[0:1, pl.ds(chunk * LANES, LANES)], (ROWS, LANES))

            def slope_y(part):
                upper = jnp.where(high, after[part][chunk + 1] if chunk + 1 < chunks else zero, after[part][chunk])
                lower = jnp.where(low, before[part][chunk - 1] if chunk else zero, before[part][chunk])
                return (upper - lower) * rate

            def slope_x(part):
                return speed(part, chunk, dx=1) - speed(part, chunk, dx=-1)

            def slope_z(part):
                return speed(part, chunk, dz=1) - speed(part, chunk, dz=-1)

            strain = [
                slope_x(0),
                slope_y(1),
                slope_z(2),
                slope_y(0) + slope_x(1),
                slope_z(0) + slope_x(2),
                slope_z(1) + slope_y(2),
            ]
            ours = [middle[part][chunk] for part in range(3)]
            square = [s * s for s in strain]
            size = root(0.5 * (square[0] + square[1] + square[2]) + 0.25 * (square[3] + square[4] + square[5]))
            pairs = [ours[0] * ours[0], ours[1] * ours[1], ours[2] * ours[2],
                     ours[0] * ours[1], ours[0] * ours[2], ours[1] * ours[2]]
            values = strain + [size * s for s in strain] + pairs + ours + [size]
            for number, value in enumerate(values):
                field[number, chunk, row + 1, pl.ds(ROWS * tile, ROWS), :] = value

    def model(row, tile):
        for chunk in range(chunks):
            def smooth(number):
                lines = []
                for k in range(4):
                    a, b, c = (field[number, chunk, row + k, pl.ds(ROWS * tile + dz, ROWS), :] for dz in range(3))
                    lines.append((a + c) + (b + b))
                pair = [lines[k] + lines[k + 1] for k in range(3)]
                return [pair[k] + pair[k + 1] for k in range(2)]

            test = [smooth(k) for k in range(6)]
            speeds = [[0.25 * s for s in smooth(18 + k)] for k in range(3)]
            scale = []
            for k in range(2):
                t = [v[k] * v[k] for v in test]
                scale.append(root((1.0 / 32.0) * (t[0] + t[1] + t[2]) + (1.0 / 64.0) * (t[3] + t[4] + t[5])))
            lm, mm_d, mm_o = [zero, zero], [zero, zero], [zero, zero]
            for number, (i, j) in enumerate(((0, 0), (1, 1), (2, 2), (0, 1), (0, 2), (1, 2))):
                stress, pairs = smooth(6 + number), smooth(12 + number)
                for k in range(2):
                    term = stress[k] - scale[k] * test[number][k]
                    lm[k] = lm[k] + (pairs[k] - speeds[i][k] * speeds[j][k]) * term
                    if number < 3:
                        mm_d[k] = mm_d[k] + term * term
                    else:
                        mm_o[k] = mm_o[k] + term * term
            lm_scale = jnp.broadcast_to(gaps[1:2, pl.ds(chunk * LANES, LANES)], (ROWS, LANES))
            mm_scale = jnp.broadcast_to(gaps[2:3, pl.ds(chunk * LANES, LANES)], (ROWS, LANES))
            lm = [lm_scale * v for v in lm]
            mm = [mm_scale * (a + 0.5 * b) for a, b in zip(mm_d, mm_o)]
            for k in range(2):
                spot = (row + k, pl.ds(ROWS * tile, ROWS), pl.ds(chunk * LANES, LANES))
                lm_out[spot] = lm[k]
                mm_out[spot] = mm[k]
            acc[chunk] += lm[0] + lm[1]
            acc[chunks + chunk] += mm[0] + mm[1]

    def over(start, stop, call, step=1):
        def turn(k, carry):
            call(start + step * k)
            return carry
        lax.fori_loop(0, (stop - start) // step, turn, 0)

    for tile in range(1, tiles - 1):
        over(1, nx - 1, lambda row, tile=tile: strains(row, tile))
    for side in sides:
        side.wait_recv()
    for tile in (0, tiles - 1, tiles):
        over(1, nx - 1, lambda row, tile=tile: strains(row, tile))
    for tile in range(tiles):
        over(2, nx - 2, lambda row, tile=tile: model(row, tile), step=2)

    edges = ((-1, 0), (nx - 1, nx))

    def edge_strains(tile):
        for pair in edges:
            over(pair[0], pair[1] + 1, lambda row: strains(row, tile))

    def edge_model(tile):
        over(0, 2 * (nx - 2), lambda row: model(row, tile), step=nx - 2)

    for strip in strips[0]:
        strip.wait_recv()
    for corner in corners_left:
        corner.start()
    for strip in strips[tiles - 1]:
        strip.wait_recv()
    for corner in corners_right:
        corner.start()
    for strip in strips[1]:
        strip.wait_recv()
    edge_strains(1)
    for corner in corners_left + corners_right:
        corner.wait_recv()
    edge_strains(0)
    edge_strains(tiles)
    edge_model(0)
    for strip in strips[2]:
        strip.wait_recv()
    edge_strains(2)
    edge_strains(3)
    for tile in range(1, tiles):
        edge_model(tile)

    for number in range(2 * chunks):
        sent[0, number : number + 1, :] = jnp.sum(acc[number], axis=0, keepdims=True)
    for number in range(2 * chunks, ROWS):
        sent[0, number : number + 1, :] = jnp.zeros((1, LANES), jnp.float32)
    mine = plane_slot(me)
    plane_in[mine] = sent[0]
    copies = []
    for number, off in enumerate(plane[1:]):
        copy = pltpu.make_async_remote_copy(
            src_ref=sent.at[0], dst_ref=plane_in.at[mine],
            send_sem=plane_send.at[number], recv_sem=plane_recv.at[mine],
            device_id=in_plane(off, 1), device_id_type=MESH,
        )
        copy.start()
        copies.append(copy)
    for off in plane[1:]:
        slot = plane_slot(in_plane(off, -1))
        pltpu.make_async_remote_copy(
            src_ref=sent.at[0], dst_ref=plane_in.at[slot],
            send_sem=plane_send.at[0], recv_sem=plane_recv.at[slot],
            device_id=in_plane(off, -1), device_id_type=MESH,
        ).wait_recv()
    total = [plane_in[k] for k in range(len(plane))]
    while len(total) > 1:
        total = [a + b for a, b in zip(total[::2], total[1::2])]
    sent[1] = total[0]
    line_in[me[0]] = total[0]
    for off in range(1, nz):
        copy = pltpu.make_async_remote_copy(
            src_ref=sent.at[1], dst_ref=line_in.at[me[0]],
            send_sem=line_send.at[off], recv_sem=line_recv.at[me[0]],
            device_id=on_line(off, 1), device_id_type=MESH,
        )
        copy.start()
        copies.append(copy)
    for off in range(1, nz):
        slot = on_line(off, -1)[0]
        pltpu.make_async_remote_copy(
            src_ref=sent.at[1], dst_ref=line_in.at[slot],
            send_sem=line_send.at[off], recv_sem=line_recv.at[slot],
            device_id=on_line(off, -1), device_id_type=MESH,
        ).wait_recv()
    total = [line_in[k] for k in range(nz)]
    while len(total) > 1:
        total = [a + b for a, b in zip(total[::2], total[1::2])]
    total = total[0]

    factors = []
    for chunk in range(chunks):
        number = pl.ds(chunk * LANES, LANES)
        share = total[chunk : chunk + 1, :] * (1.0 / planes)
        base = total[chunks + chunk : chunks + chunk + 1, :] * (1.0 / planes) + 1e-06
        coefficient = share / base
        coef_out[0:1, number] = coefficient
        factors.append(jnp.broadcast_to(coefficient * gaps[3:4, number], (ROWS, LANES)))

    def viscosity(row):
        for tile in range(tiles):
            for chunk in range(chunks):
                size = field[21, chunk, row + 1, pl.ds(ROWS * tile + 1, ROWS), :]
                eddy[row, pl.ds(ROWS * tile, ROWS), pl.ds(chunk * LANES, LANES)] = factors[chunk] * size

    over(0, nx, viscosity)
    for copy in sides + [s for pair in strips for s in pair] + corners_left + corners_right + copies:
        copy.wait_send()


def solution(mesh):
    shape = (8, 2, 4, 2, 2)
    torus = Mesh(mesh.devices.reshape(shape), AXES)

    def per_device(velocity, y_gap):
        _, nx, depth, height = velocity.shape
        chunks, tiles = height // LANES, depth // ROWS
        cells = nx * lax.axis_size(GX) * depth * lax.axis_size(GZ)
        span = y_gap[:-1] + y_gap[1:]
        width_sq = (0.5 * span) ** (2.0 / 3.0)
        gaps = jnp.stack([2.0 / span, width_sq * (1.0 / 256.0), width_sq * width_sq * (1.0 / 256.0), width_sq])
        rims = 2 + 2 * tiles + 4
        in_plane = shape[1] * shape[2] * shape[3] * shape[4]
        grid = jax.ShapeDtypeStruct((nx, depth, height), jnp.float32)
        vmem = pl.BlockSpec(memory_space=pltpu.VMEM)
        eddy, lm, mm, coefficient = pl.pallas_call(
            lambda *refs: kernel(shape, cells, *refs),
            out_shape=(grid, grid, grid, jax.ShapeDtypeStruct((1, height), jnp.float32)),
            in_specs=[pl.BlockSpec(memory_space=pltpu.HBM), vmem],
            out_specs=(vmem, vmem, vmem, vmem),
            scratch_shapes=[
                pltpu.VMEM((3, chunks, nx + 4, depth + 16, LANES), jnp.float32),
                pltpu.VMEM((22, chunks, nx + 2, depth + 8, LANES), jnp.float32),
                pltpu.VMEM((2 * chunks, ROWS, LANES), jnp.float32),
                pltpu.VMEM((2, ROWS, LANES), jnp.float32),
                pltpu.VMEM((in_plane, ROWS, LANES), jnp.float32),
                pltpu.VMEM((shape[0], ROWS, LANES), jnp.float32),
                pltpu.SemaphoreType.DMA((3 * chunks,)),
                pltpu.SemaphoreType.DMA((rims,)),
                pltpu.SemaphoreType.DMA((rims,)),
                pltpu.SemaphoreType.DMA((in_plane,)),
                pltpu.SemaphoreType.DMA((in_plane,)),
                pltpu.SemaphoreType.DMA((shape[0],)),
                pltpu.SemaphoreType.DMA((shape[0],)),
            ],
            compiler_params=pltpu.CompilerParams(
                collective_id=0, has_side_effects=True, vmem_limit_bytes=40 * 1024 * 1024
            ),
            name="smagorinsky",
        )(velocity, gaps)
        return eddy, lm, mm, coefficient[0]

    return jax.shard_map(
        per_device,
        mesh=torus,
        in_specs=(P(None, GX, GZ, None), P()),
        out_specs=(P(GX, GZ, None), P(GX, GZ, None), P(GX, GZ, None), P()),
        check_vma=False,
    )
```

```python
import jax
import jax.numpy as jnp
from jax import lax
from jax.experimental import pallas as pl
from jax.experimental.pallas import tpu as pltpu
from jax.sharding import Mesh
from jax.sharding import PartitionSpec as P

AXES = ("gx_0", "gx_1", "gz_0", "gz_1", "gz_2")
GX = ("gx_0", "gx_1")
GZ = ("gz_0", "gz_1", "gz_2")
MESH = pl.DeviceIdType.MESH

LANES = 128
ROWS = 8
TINY = 1.1754944e-38


def root(square):
    return square * lax.rsqrt(jnp.maximum(square, TINY))


def kernel(sizes, planes, vel, y_gap, size_out, lm_out, mm_out, coef_out, pad, field, gap, last, gaps, acc, sent, got,
           load_sem, send_sem, recv_sem, sum_send, sum_recv):
    nz, nxl, ny, nxh, nc = sizes
    nx, depth = vel.shape[1], vel.shape[2]
    chunks = vel.shape[3] // LANES
    tiles = depth // ROWS
    me = tuple(lax.axis_index(name) for name in AXES)

    loads = []
    for part in range(3):
        for chunk in range(chunks):
            loads.append(
                pltpu.make_async_copy(
                    vel.at[part, :, :, pl.ds(chunk * LANES, LANES)],
                    pad.at[part, chunk, pl.ds(2, nx), pl.ds(2, depth), :],
                    load_sem.at[part * chunks + chunk],
                )
            )
    loads.append(pltpu.make_async_copy(y_gap.at[pl.ds(0, chunks * LANES)], gap, load_sem.at[3 * chunks]))
    loads.append(pltpu.make_async_copy(y_gap, last, load_sem.at[3 * chunks + 1]))

    def along_x(step):
        ring = nz * nxl
        spot = lax.rem(me[0] * nxl + me[1] + step + ring, ring)
        return (spot // nxl, lax.rem(spot, nxl), me[2], me[3], me[4])

    def along_z(step):
        ring = ny * nxh * nc
        spot = lax.rem((me[2] * nxh + me[3]) * nc + me[4] + step + ring, ring)
        return (me[0], me[1], spot // (nxh * nc), lax.rem(spot // nc, nxh), lax.rem(spot, nc))

    def around(gx_step, gz_step):
        z, xl, *_ = along_x(gx_step)
        return (z, xl, *along_z(gz_step)[2:])

    def near(off, sign):
        xl, xh, c = (lax.rem(m + sign * o + n, n) for m, o, n in zip((me[1], me[3], me[4]), off, (nxl, nxh, nc)))
        return (me[0], xl, me[2], xh, c)

    def on_y(off, sign):
        return (me[0], me[1], lax.rem(me[2] + sign * off + ny, ny), me[3], me[4])

    def on_z(off, sign):
        return (lax.rem(me[0] + sign * off + nz, nz), *me[1:])

    group = [(a, b, c) for a in range(nxl) for b in range(nxh) for c in range(nc)]
    stages = (
        (near, group[1:], lambda spot: (spot[1] * nxh + spot[3]) * nc + spot[4], len(group)),
        (on_y, range(1, ny), lambda spot: spot[2], ny),
        (on_z, range(1, nz), lambda spot: spot[0], nz),
    )

    barrier = pltpu.get_barrier_semaphore()
    steps = [(1, 0), (-1, 0), (0, 1), (0, -1), (1, 1), (1, -1), (-1, 1), (-1, -1)]
    greeted = [around(*step) for step in steps] + [to(off, 1) for to, offs, _, _ in stages for off in offs]
    for other in greeted:
        pl.semaphore_signal(barrier, inc=1, device_id=other, device_id_type=MESH)
    for load in loads:
        load.start()
    acc[...] = jnp.zeros_like(acc)
    for load in loads:
        load.wait()
    pl.semaphore_wait(barrier, len(greeted))

    def rim(number, source, target, other):
        return pltpu.make_async_remote_copy(
            src_ref=pad.at[:, :, pl.ds(*source[0]), pl.ds(*source[1]), :],
            dst_ref=pad.at[:, :, pl.ds(*target[0]), pl.ds(*target[1]), :],
            send_sem=send_sem.at[number],
            recv_sem=recv_sem.at[number],
            device_id=other,
            device_id_type=MESH,
        )

    up, down, right, left = along_x(1), along_x(-1), along_z(1), along_z(-1)
    body = (2, nx)
    sides = [
        rim(0, (body, (depth, 2)), (body, (0, 2)), right),
        rim(1, (body, (2, 2)), (body, (depth + 2, 2)), left),
    ]
    strips = []
    for tile in range(tiles):
        cut = (2 + ROWS * tile, ROWS)
        strips.append((
            rim(2 + 2 * tile, ((nx, 2), cut), ((0, 2), cut), up),
            rim(3 + 2 * tile, ((2, 2), cut), ((nx + 2, 2), cut), down),
        ))
    first = 2 + 2 * tiles
    corners = [
        rim(first, ((nx, 2), (depth, 2)), ((0, 2), (0, 2)), around(1, 1)),
        rim(first + 1, ((nx, 2), (2, 2)), ((0, 2), (depth + 2, 2)), around(1, -1)),
        rim(first + 2, ((2, 2), (depth, 2)), ((nx + 2, 2), (0, 2)), around(-1, 1)),
        rim(first + 3, ((2, 2), (2, 2)), ((nx + 2, 2), (depth + 2, 2)), around(-1, -1)),
    ]

    for copy in sides + corners + [strip for pair in strips for strip in pair]:
        copy.start()

    lane = lax.broadcasted_iota(jnp.int32, (ROWS, LANES), 1)
    low, high = lane == 0, lane == LANES - 1
    zero = jnp.zeros((ROWS, LANES), jnp.float32)
    for chunk in range(chunks):
        line = pl.ds(chunk * LANES, LANES)
        here = gap[line].reshape(1, LANES)
        if chunk + 1 < chunks:
            then = gap[pl.ds((chunk + 1) * LANES, LANES)].reshape(1, LANES)
        else:
            then = last[chunks * LANES]
        after = pltpu.roll(jnp.where(low[:1], then, here), LANES - 1, 1)
        span = here + after
        width_sq = jnp.exp((2.0 / 3.0) * jnp.log(0.5 * span))
        gaps[0:1, line] = 2.0 / span
        gaps[1:2, line] = width_sq * (1.0 / 256.0)
        gaps[2:3, line] = width_sq * width_sq * (1.0 / 256.0)
        gaps[3:4, line] = width_sq

    def strains(row, tile):
        here, at = row + 2, ROWS * tile + 1

        def speed(part, chunk, dx=0, dz=0):
            return pad[part, chunk, here + dx, pl.ds(at + dz, ROWS), :]

        middle = [[speed(part, chunk) for chunk in range(chunks)] for part in range(3)]
        before = [[pltpu.roll(v, 1, 1) for v in parts] for parts in middle]
        after = [[pltpu.roll(v, LANES - 1, 1) for v in parts] for parts in middle]
        for chunk in range(chunks):
            rate = jnp.broadcast_to(gaps[0:1, pl.ds(chunk * LANES, LANES)], (ROWS, LANES))

            def slope_y(part):
                upper = jnp.where(high, after[part][chunk + 1] if chunk + 1 < chunks else zero, after[part][chunk])
                lower = jnp.where(low, before[part][chunk - 1] if chunk else zero, before[part][chunk])
                return (upper - lower) * rate

            def slope_x(part):
                return speed(part, chunk, dx=1) - speed(part, chunk, dx=-1)

            def slope_z(part):
                return speed(part, chunk, dz=1) - speed(part, chunk, dz=-1)

            strain = [
                slope_x(0),
                slope_y(1),
                slope_z(2),
                slope_y(0) + slope_x(1),
                slope_z(0) + slope_x(2),
                slope_z(1) + slope_y(2),
            ]
            ours = [middle[part][chunk] for part in range(3)]
            square = [s * s for s in strain]
            size = root(0.5 * (square[0] + square[1] + square[2]) + 0.25 * (square[3] + square[4] + square[5]))
            pairs = [ours[0] * ours[0], ours[1] * ours[1], ours[2] * ours[2],
                     ours[0] * ours[1], ours[0] * ours[2], ours[1] * ours[2]]
            values = strain + [size * s for s in strain] + pairs + ours + [size]
            for number, value in enumerate(values):
                field[number, chunk, row + 1, pl.ds(ROWS * tile, ROWS), :] = value

    def model(row, tile):
        for chunk in range(chunks):
            def smooth(number):
                lines = []
                for k in range(4):
                    a, b, c = (field[number, chunk, row + k, pl.ds(ROWS * tile + dz, ROWS), :] for dz in range(3))
                    lines.append((a + c) + (b + b))
                pair = [lines[k] + lines[k + 1] for k in range(3)]
                return [pair[k] + pair[k + 1] for k in range(2)]

            test = [smooth(k) for k in range(6)]
            speeds = [[0.25 * s for s in smooth(18 + k)] for k in range(3)]
            scale = []
            for k in range(2):
                t = [v[k] * v[k] for v in test]
                scale.append(root((1.0 / 32.0) * (t[0] + t[1] + t[2]) + (1.0 / 64.0) * (t[3] + t[4] + t[5])))
            lm, mm_d, mm_o = [zero, zero], [zero, zero], [zero, zero]
            for number, (i, j) in enumerate(((0, 0), (1, 1), (2, 2), (0, 1), (0, 2), (1, 2))):
                stress, pairs = smooth(6 + number), smooth(12 + number)
                for k in range(2):
                    term = stress[k] - scale[k] * test[number][k]
                    lm[k] = lm[k] + (pairs[k] - speeds[i][k] * speeds[j][k]) * term
                    if number < 3:
                        mm_d[k] = mm_d[k] + term * term
                    else:
                        mm_o[k] = mm_o[k] + term * term
            lm_scale = jnp.broadcast_to(gaps[1:2, pl.ds(chunk * LANES, LANES)], (ROWS, LANES))
            mm_scale = jnp.broadcast_to(gaps[2:3, pl.ds(chunk * LANES, LANES)], (ROWS, LANES))
            lm = [lm_scale * v for v in lm]
            mm = [mm_scale * (a + 0.5 * b) for a, b in zip(mm_d, mm_o)]
            for k in range(2):
                spot = (row + k, pl.ds(ROWS * tile, ROWS), pl.ds(chunk * LANES, LANES))
                size_out[spot] = field[21, chunk, row + k + 1, pl.ds(ROWS * tile + 1, ROWS), :]
                lm_out[spot] = lm[k]
                mm_out[spot] = mm[k]
            acc[chunk] += lm[0] + lm[1]
            acc[chunks + chunk] += mm[0] + mm[1]

    def over(start, stop, call, step=1):
        def turn(k, carry):
            call(start + step * k)
            return carry
        lax.fori_loop(0, (stop - start) // step, turn, 0)

    for tile in range(1, tiles - 1):
        over(1, nx - 1, lambda row, tile=tile: strains(row, tile))
    for side in sides:
        side.wait_recv()
    for tile in (0, tiles - 1, tiles):
        over(1, nx - 1, lambda row, tile=tile: strains(row, tile))
    for tile in range(tiles):
        over(2, nx - 2, lambda row, tile=tile: model(row, tile), step=2)

    edges = ((-1, 0, 0), (nx - 1, nx - 1, nx - 2))
    for tile in range(tiles + 1):
        for side, (start, _, block) in enumerate(edges):
            if tile == 0:
                corners[2 * side].wait_recv()
                corners[2 * side + 1].wait_recv()
            if tile < tiles:
                strips[tile][side].wait_recv()
            over(start, start + 2, lambda row, tile=tile: strains(row, tile))
            if tile:
                model(block, tile - 1)

    for number in range(2 * chunks):
        sent[0, number : number + 1, :] = jnp.sum(acc[number], axis=0, keepdims=True)
    for number in range(2 * chunks, ROWS):
        sent[0, number : number + 1, :] = jnp.zeros((1, LANES), jnp.float32)
    total = sent[0]
    copies, base = [], 0
    for number, (to, offs, slot_of, count) in enumerate(stages):
        if number:
            sent[number] = total
        mine = base + slot_of(me)
        got[mine] = total
        for off in offs:
            copy = pltpu.make_async_remote_copy(
                src_ref=sent.at[number], dst_ref=got.at[mine],
                send_sem=sum_send.at[len(copies)], recv_sem=sum_recv.at[mine],
                device_id=to(off, 1), device_id_type=MESH,
            )
            copy.start()
            copies.append(copy)
        for off in offs:
            other = to(off, -1)
            slot = base + slot_of(other)
            pltpu.make_async_remote_copy(
                src_ref=sent.at[number], dst_ref=got.at[slot],
                send_sem=sum_send.at[0], recv_sem=sum_recv.at[slot],
                device_id=other, device_id_type=MESH,
            ).wait_recv()
        terms = [got[base + k] for k in range(count)]
        while len(terms) > 1:
            terms = [a + b for a, b in zip(terms[::2], terms[1::2])]
        total = terms[0]
        base += count

    for chunk in range(chunks):
        line = pl.ds(chunk * LANES, LANES)
        share = total[chunk : chunk + 1, :] * (1.0 / planes)
        below = total[chunks + chunk : chunks + chunk + 1, :] * (1.0 / planes) + 1e-06
        coefficient = share / below
        coef_out[0:1, line] = coefficient
        coef_out[1:2, line] = coefficient * gaps[3:4, line]
    for copy in sides + corners + [strip for pair in strips for strip in pair] + copies:
        copy.wait_send()


def finish(size, lm, mm, coef, eddy_out, lm_out, mm_out, coef_out, eddy, sem):
    copies = [
        pltpu.make_async_copy(lm, lm_out, sem.at[0]),
        pltpu.make_async_copy(mm, mm_out, sem.at[1]),
        pltpu.make_async_copy(coef.at[0], coef_out, sem.at[2]),
        pltpu.make_async_copy(eddy, eddy_out, sem.at[3]),
    ]
    for copy in copies[:3]:
        copy.start()
    eddy[...] = size[...] * coef[1:2, :].reshape(1, 1, coef.shape[1])
    copies[3].start()
    for copy in copies:
        copy.wait()


def solution(mesh):
    shape = (8, 2, 4, 2, 2)
    torus = Mesh(mesh.devices.reshape(shape), AXES)

    def per_device(velocity, y_gap):
        _, nx, depth, height = velocity.shape
        chunks, tiles = height // LANES, depth // ROWS
        cells = nx * lax.axis_size(GX) * depth * lax.axis_size(GZ)
        rims = 2 + 2 * tiles + 4
        ways = shape[1] * shape[3] * shape[4] + shape[2] + shape[0]
        grid = jax.ShapeDtypeStruct((nx, depth, height), jnp.float32)
        vmem = pl.BlockSpec(memory_space=pltpu.VMEM)
        hbm = pl.BlockSpec(memory_space=pltpu.HBM)
        size, lm, mm, coefficient = pl.pallas_call(
            lambda *refs: kernel(shape, cells, *refs),
            out_shape=(grid, grid, grid, jax.ShapeDtypeStruct((2, height), jnp.float32)),
            in_specs=[hbm, hbm],
            out_specs=(vmem, vmem, vmem, vmem),
            scratch_shapes=[
                pltpu.VMEM((3, chunks, nx + 4, depth + 16, LANES), jnp.float32),
                pltpu.VMEM((22, chunks, nx + 2, depth + 8, LANES), jnp.float32),
                pltpu.VMEM((height,), jnp.float32),
                pltpu.SMEM((height + 1,), jnp.float32),
                pltpu.VMEM((4, height), jnp.float32),
                pltpu.VMEM((2 * chunks, ROWS, LANES), jnp.float32),
                pltpu.VMEM((3, ROWS, LANES), jnp.float32),
                pltpu.VMEM((ways, ROWS, LANES), jnp.float32),
                pltpu.SemaphoreType.DMA((3 * chunks + 2,)),
                pltpu.SemaphoreType.DMA((rims,)),
                pltpu.SemaphoreType.DMA((rims,)),
                pltpu.SemaphoreType.DMA((ways,)),
                pltpu.SemaphoreType.DMA((ways,)),
            ],
            compiler_params=pltpu.CompilerParams(
                collective_id=0, has_side_effects=True, vmem_limit_bytes=40 * 1024 * 1024
            ),
            name="smagorinsky",
        )(pltpu.with_memory_space_constraint(velocity, pltpu.HBM), pltpu.with_memory_space_constraint(y_gap, pltpu.HBM))
        return pl.pallas_call(
            finish,
            out_shape=(grid, grid, grid, jax.ShapeDtypeStruct((height,), jnp.float32)),
            in_specs=[vmem] * 4,
            out_specs=[hbm] * 4,
            scratch_shapes=[pltpu.VMEM((nx, depth, height), jnp.float32), pltpu.SemaphoreType.DMA((4,))],
            compiler_params=pltpu.CompilerParams(vmem_limit_bytes=4 * 1024 * 1024),
            name="finish",
        )(size, lm, mm, coefficient)

    return jax.shard_map(
        per_device,
        mesh=torus,
        in_specs=(P(None, GX, GZ, None), P()),
        out_specs=(P(GX, GZ, None), P(GX, GZ, None), P(GX, GZ, None), P()),
        check_vma=False,
    )
```

```python
import itertools
import math

import jax
import jax.numpy as jnp
from jax import lax
from jax.experimental import pallas as pl
from jax.experimental.pallas import tpu as pltpu
from jax.sharding import Mesh
from jax.sharding import PartitionSpec as P

AXES = ("gx_0", "gx_1", "gz_0", "gz_1", "gz_2")
GX = ("gx_0", "gx_1")
GZ = ("gz_0", "gz_1", "gz_2")
MESH = pl.DeviceIdType.MESH

LANES = 128
ROWS = 8
STAGES = ((4,), (1, 2, 3), (0,))
OFFSET = 8
AHEAD = 6
CUTS = (0, 11, 19, 27)
TINY = 1.1754944e-38


def root(square):
    return square * lax.rsqrt(jnp.maximum(square, TINY))


def kernel(sizes, planes, vel, y_gap, size_out, lm_out, mm_out, coef_out, pad, field, gap, last, gaps, acc, sent, got,
           load_sem, send_sem, recv_sem, sum_send, sum_recv):
    nz, nxl, ny, nxh, nc = sizes
    nx, depth = vel.shape[1], vel.shape[2]
    chunks = vel.shape[3] // LANES
    tiles = depth // ROWS
    me = tuple(lax.axis_index(name) for name in AXES)

    loads = []
    for part in range(3):
        for chunk in range(chunks):
            loads.append(
                pltpu.make_async_copy(
                    vel.at[part, :, :, pl.ds(chunk * LANES, LANES)],
                    pad.at[part, chunk, pl.ds(2, nx), pl.ds(OFFSET, depth), :],
                    load_sem.at[part * chunks + chunk],
                )
            )
    loads.append(pltpu.make_async_copy(y_gap.at[pl.ds(0, chunks * LANES)], gap, load_sem.at[3 * chunks]))
    loads.append(pltpu.make_async_copy(y_gap, last, load_sem.at[3 * chunks + 1]))
    for load in loads:
        load.start()

    def along_x(step):
        ring = nz * nxl
        spot = lax.rem(me[0] * nxl + me[1] + step + ring, ring)
        return (spot // nxl, lax.rem(spot, nxl), me[2], me[3], me[4])

    def along_z(step):
        ring = ny * nxh * nc
        spot = lax.rem((me[2] * nxh + me[3]) * nc + me[4] + step + ring, ring)
        return (me[0], me[1], spot // (nxh * nc), lax.rem(spot // nc, nxh), lax.rem(spot, nc))

    def around(gx_step, gz_step):
        z, xl, *_ = along_x(gx_step)
        return (z, xl, *along_z(gz_step)[2:])

    def shifted(axes, off, sign):
        spot = list(me)
        for axis, step in zip(axes, off):
            spot[axis] = lax.rem(me[axis] + sign * step + sizes[axis], sizes[axis])
        return tuple(spot)

    def slot_of(axes, spot):
        slot = 0
        for axis in axes:
            slot = slot * sizes[axis] + spot[axis]
        return slot

    stages = [(axes, list(itertools.product(*(range(sizes[axis]) for axis in axes)))) for axes in STAGES]

    barrier = pltpu.get_barrier_semaphore()
    steps = [(1, 0), (-1, 0), (0, 1), (0, -1), (1, 1), (1, -1), (-1, 1), (-1, -1)]
    greeted = [around(*step) for step in steps] + [shifted(axes, off, 1) for axes, offs in stages for off in offs[1:]]
    for other in greeted:
        pl.semaphore_signal(barrier, inc=1, device_id=other, device_id_type=MESH)
    acc[...] = jnp.zeros_like(acc)
    for load in loads:
        load.wait()
    pl.semaphore_wait(barrier, len(greeted))

    def rim(number, source, target, other):
        return pltpu.make_async_remote_copy(
            src_ref=pad.at[:, :, pl.ds(*source[0]), pl.ds(*source[1]), :],
            dst_ref=pad.at[:, :, pl.ds(*target[0]), pl.ds(*target[1]), :],
            send_sem=send_sem.at[number],
            recv_sem=recv_sem.at[number],
            device_id=other,
            device_id_type=MESH,
        )

    up, down, right, left = along_x(1), along_x(-1), along_z(1), along_z(-1)
    body = (2, nx)
    first_two, last_two = (OFFSET, 2), (OFFSET + depth - 2, 2)
    before, behind = (OFFSET - 2, 2), (OFFSET + depth, 2)
    sides = [
        rim(0, (body, last_two), (body, before), right),
        rim(1, (body, first_two), (body, behind), left),
    ]
    strips = []
    cuts = [(OFFSET + a, b - a) for a, b in zip(CUTS, CUTS[1:] + (depth,))]
    for number, cut in enumerate(cuts):
        strips.append((
            rim(2 + 2 * number, ((nx, 2), cut), ((0, 2), cut), up),
            rim(3 + 2 * number, ((2, 2), cut), ((nx + 2, 2), cut), down),
        ))
    first = 2 + 2 * len(cuts)
    corners = [
        rim(first, ((nx, 2), last_two), ((0, 2), before), around(1, 1)),
        rim(first + 1, ((nx, 2), first_two), ((0, 2), behind), around(1, -1)),
        rim(first + 2, ((2, 2), last_two), ((nx + 2, 2), before), around(-1, 1)),
        rim(first + 3, ((2, 2), first_two), ((nx + 2, 2), behind), around(-1, -1)),
    ]

    for copy in sides + corners:
        copy.start()

    lane = lax.broadcasted_iota(jnp.int32, (ROWS, LANES), 1)
    low, high = lane == 0, lane == LANES - 1
    zero = jnp.zeros((ROWS, LANES), jnp.float32)
    for chunk in range(chunks):
        line = pl.ds(chunk * LANES, LANES)
        here = gap[line].reshape(1, LANES)
        if chunk + 1 < chunks:
            then = gap[pl.ds((chunk + 1) * LANES, LANES)].reshape(1, LANES)
        else:
            then = last[chunks * LANES]
        after = pltpu.roll(jnp.where(low[:1], then, here), LANES - 1, 1)
        span = here + after
        width_sq = jnp.exp((2.0 / 3.0) * jnp.log(0.5 * span))
        gaps[0:1, line] = 2.0 / span
        gaps[1:2, line] = width_sq * (1.0 / 256.0)
        gaps[2:3, line] = width_sq * width_sq * (1.0 / 256.0)
        gaps[3:4, line] = width_sq

    def strains(row, tile):
        here, at = row + 2, ROWS * tile - AHEAD + OFFSET

        def speed(part, chunk, dx=0, dz=0):
            return pad[part, chunk, here + dx, pl.ds(at + dz, ROWS), :]

        middle = [[speed(part, chunk) for chunk in range(chunks)] for part in range(3)]
        before = [[pltpu.roll(v, 1, 1) for v in parts] for parts in middle]
        after = [[pltpu.roll(v, LANES - 1, 1) for v in parts] for parts in middle]
        for chunk in range(chunks):
            rate = jnp.broadcast_to(gaps[0:1, pl.ds(chunk * LANES, LANES)], (ROWS, LANES))

            def slope_y(part):
                upper = jnp.where(high, after[part][chunk + 1] if chunk + 1 < chunks else zero, after[part][chunk])
                lower = jnp.where(low, before[part][chunk - 1] if chunk else zero, before[part][chunk])
                return (upper - lower) * rate

            def slope_x(part):
                return speed(part, chunk, dx=1) - speed(part, chunk, dx=-1)

            def slope_z(part):
                return speed(part, chunk, dz=1) - speed(part, chunk, dz=-1)

            strain = [
                slope_x(0),
                slope_y(1),
                slope_z(2),
                slope_y(0) + slope_x(1),
                slope_z(0) + slope_x(2),
                slope_z(1) + slope_y(2),
            ]
            ours = [middle[part][chunk] for part in range(3)]
            square = [s * s for s in strain]
            size = root(0.5 * (square[0] + square[1] + square[2]) + 0.25 * (square[3] + square[4] + square[5]))
            pairs = [ours[0] * ours[0], ours[1] * ours[1], ours[2] * ours[2],
                     ours[0] * ours[1], ours[0] * ours[2], ours[1] * ours[2]]
            values = strain + [size * s for s in strain] + pairs + ours + [size]
            for number, value in enumerate(values):
                field[number, chunk, row + 1, pl.ds(ROWS * tile, ROWS), :] = value

    def model(row, tile):
        for chunk in range(chunks):
            def smooth(number):
                lines = []
                for k in range(4):
                    a, b, c = (field[number, chunk, row + k, pl.ds(ROWS * tile + AHEAD + dz, ROWS), :] for dz in (-1, 0, 1))
                    lines.append((a + c) + (b + b))
                pair = [lines[k] + lines[k + 1] for k in range(3)]
                return [pair[k] + pair[k + 1] for k in range(2)]

            test = [smooth(k) for k in range(6)]
            speeds = [[0.25 * s for s in smooth(18 + k)] for k in range(3)]
            scale = []
            for k in range(2):
                t = [v[k] * v[k] for v in test]
                scale.append(root((1.0 / 32.0) * (t[0] + t[1] + t[2]) + (1.0 / 64.0) * (t[3] + t[4] + t[5])))
            lm, mm_d, mm_o = [zero, zero], [zero, zero], [zero, zero]
            for number, (i, j) in enumerate(((0, 0), (1, 1), (2, 2), (0, 1), (0, 2), (1, 2))):
                stress, pairs = smooth(6 + number), smooth(12 + number)
                for k in range(2):
                    term = stress[k] - scale[k] * test[number][k]
                    lm[k] = lm[k] + (pairs[k] - speeds[i][k] * speeds[j][k]) * term
                    if number < 3:
                        mm_d[k] = mm_d[k] + term * term
                    else:
                        mm_o[k] = mm_o[k] + term * term
            lm_scale = jnp.broadcast_to(gaps[1:2, pl.ds(chunk * LANES, LANES)], (ROWS, LANES))
            mm_scale = jnp.broadcast_to(gaps[2:3, pl.ds(chunk * LANES, LANES)], (ROWS, LANES))
            lm = [lm_scale * v for v in lm]
            mm = [mm_scale * (a + 0.5 * b) for a, b in zip(mm_d, mm_o)]
            for k in range(2):
                spot = (row + k, pl.ds(ROWS * tile, ROWS), pl.ds(chunk * LANES, LANES))
                size_out[spot] = field[21, chunk, row + k + 1, pl.ds(ROWS * tile + AHEAD, ROWS), :]
                lm_out[spot] = lm[k]
                mm_out[spot] = mm[k]
            acc[chunk] += lm[0] + lm[1]
            acc[chunks + chunk] += mm[0] + mm[1]

    def over(start, stop, call, step=1):
        def turn(k, carry):
            call(start + step * k)
            return carry
        lax.fori_loop(0, (stop - start) // step, turn, 0)

    over(1, nx - 1, lambda row: strains(row, 1))
    for side in sides:
        side.wait_send()
    for pair in strips:
        for strip in pair:
            strip.start()
    for tile in range(2, tiles):
        over(1, nx - 1, lambda row, tile=tile: strains(row, tile))
    for side in sides:
        side.wait_recv()
    for tile in (0, tiles):
        over(1, nx - 1, lambda row, tile=tile: strains(row, tile))
    for tile in range(tiles):
        over(2, nx - 2, lambda row, tile=tile: model(row, tile), step=2)

    for turn in range(2):
        side = me[1] if turn == 0 else 1 - me[1]
        rows, start, block = side * (nx + 2), side * nx - 1, side * (nx - 2)

        def landed(number, cut):
            there = pad.at[:, :, pl.ds(rows, 2), pl.ds(*cut), :]
            pltpu.make_async_copy(there, there, recv_sem.at[number]).wait()

        landed(first + 2 * side, before)
        for tile in range(tiles + 1):
            if tile != 1:
                landed(2 + 2 * max(tile - 1, 0) + side, cuts[max(tile - 1, 0)])
            if tile == tiles:
                landed(first + 1 + 2 * side, behind)
            over(0, 2, lambda row, tile=tile: strains(start + row, tile))
            if tile:
                model(block, tile - 1)

    for number in range(2 * chunks):
        sent[0, number : number + 1, :] = jnp.sum(acc[number], axis=0, keepdims=True)
    for number in range(2 * chunks, ROWS):
        sent[0, number : number + 1, :] = jnp.zeros((1, LANES), jnp.float32)
    total = sent[0]
    held, messages, base = 2 * chunks, 0, 0
    for number, (axes, offs) in enumerate(stages):
        if number:
            sent[number] = total
        mine = base + slot_of(axes, me)
        for off in offs[1:]:
            pltpu.make_async_remote_copy(
                src_ref=sent.at[number, pl.ds(0, held)], dst_ref=got.at[mine, pl.ds(0, held)],
                send_sem=sum_send.at[0], recv_sem=sum_recv.at[number],
                device_id=shifted(axes, off, 1), device_id_type=MESH,
            ).start()
        got[mine] = total
        others = got.at[pl.ds(base, len(offs) - 1), pl.ds(0, held)]
        pltpu.make_async_copy(others, others, sum_recv.at[number]).wait()
        terms = [got[base + k] for k in range(len(offs))]
        while len(terms) > 1:
            terms = [a + b for a, b in zip(terms[::2], terms[1::2])]
        total = terms[0]
        base += len(offs)
        messages += len(offs) - 1

    for chunk in range(chunks):
        line = pl.ds(chunk * LANES, LANES)
        share = total[chunk : chunk + 1, :] * (1.0 / planes)
        below = total[chunks + chunk : chunks + chunk + 1, :] * (1.0 / planes) + 1e-06
        coefficient = share / below
        coef_out[0:1, line] = coefficient
        coef_out[1:2, line] = coefficient * gaps[3:4, line]
    for copy in corners + [strip for pair in strips for strip in pair]:
        copy.wait_send()
    others = got.at[pl.ds(0, messages), pl.ds(0, held)]
    pltpu.make_async_copy(others, others, sum_send.at[0]).wait()


def finish(size, lm, mm, coef, eddy_out, lm_out, mm_out, coef_out, eddy, sem):
    copies = [
        pltpu.make_async_copy(lm, lm_out, sem.at[0]),
        pltpu.make_async_copy(mm, mm_out, sem.at[1]),
        pltpu.make_async_copy(coef.at[0], coef_out, sem.at[2]),
        pltpu.make_async_copy(eddy, eddy_out, sem.at[3]),
    ]
    for copy in copies[:3]:
        copy.start()
    eddy[...] = size[...] * coef[1:2, :].reshape(1, 1, coef.shape[1])
    copies[3].start()
    for copy in copies:
        copy.wait()


def solution(mesh):
    shape = (8, 2, 4, 2, 2)
    torus = Mesh(mesh.devices.reshape(shape), AXES)

    def per_device(velocity, y_gap):
        _, nx, depth, height = velocity.shape
        chunks, tiles = height // LANES, depth // ROWS
        cells = nx * lax.axis_size(GX) * depth * lax.axis_size(GZ)
        rims = 2 + 2 * len(CUTS) + 4
        ways = sum(math.prod(shape[axis] for axis in axes) for axes in STAGES)
        grid = jax.ShapeDtypeStruct((nx, depth, height), jnp.float32)
        vmem = pl.BlockSpec(memory_space=pltpu.VMEM)
        hbm = pl.BlockSpec(memory_space=pltpu.HBM)
        size, lm, mm, coefficient = pl.pallas_call(
            lambda *refs: kernel(shape, cells, *refs),
            out_shape=(grid, grid, grid, jax.ShapeDtypeStruct((2, height), jnp.float32)),
            in_specs=[hbm, hbm],
            out_specs=(vmem, vmem, vmem, vmem),
            scratch_shapes=[
                pltpu.VMEM((3, chunks, nx + 4, depth + 16, LANES), jnp.float32),
                pltpu.VMEM((22, chunks, nx + 2, depth + 8, LANES), jnp.float32),
                pltpu.VMEM((height,), jnp.float32),
                pltpu.SMEM((height + 1,), jnp.float32),
                pltpu.VMEM((4, height), jnp.float32),
                pltpu.VMEM((2 * chunks, ROWS, LANES), jnp.float32),
                pltpu.VMEM((len(STAGES), ROWS, LANES), jnp.float32),
                pltpu.VMEM((ways, ROWS, LANES), jnp.float32),
                pltpu.SemaphoreType.DMA((3 * chunks + 2,)),
                pltpu.SemaphoreType.DMA((rims,)),
                pltpu.SemaphoreType.DMA((rims,)),
                pltpu.SemaphoreType.DMA((1,)),
                pltpu.SemaphoreType.DMA((len(STAGES),)),
            ],
            compiler_params=pltpu.CompilerParams(
                collective_id=0, has_side_effects=True, vmem_limit_bytes=40 * 1024 * 1024
            ),
            name="smagorinsky",
        )(pltpu.with_memory_space_constraint(velocity, pltpu.HBM), pltpu.with_memory_space_constraint(y_gap, pltpu.HBM))
        return pl.pallas_call(
            finish,
            out_shape=(grid, grid, grid, jax.ShapeDtypeStruct((height,), jnp.float32)),
            in_specs=[vmem] * 4,
            out_specs=[hbm] * 4,
            scratch_shapes=[pltpu.VMEM((nx, depth, height), jnp.float32), pltpu.SemaphoreType.DMA((4,))],
            compiler_params=pltpu.CompilerParams(vmem_limit_bytes=4 * 1024 * 1024),
            name="finish",
        )(size, lm, mm, coefficient)

    return jax.shard_map(
        per_device,
        mesh=torus,
        in_specs=(P(None, GX, GZ, None), P()),
        out_specs=(P(GX, GZ, None), P(GX, GZ, None), P(GX, GZ, None), P()),
        check_vma=False,
    )
```

```python
import itertools

import jax
import jax.numpy as jnp
from jax import lax
from jax.experimental import pallas as pl
from jax.experimental.pallas import tpu as pltpu
from jax.sharding import Mesh
from jax.sharding import PartitionSpec as P

AXES = ("gx_0", "gx_1", "gz_0", "gz_1", "gz_2")
GX = ("gx_0", "gx_1")
GZ = ("gz_0", "gz_1", "gz_2")
MESH = pl.DeviceIdType.MESH

LANES = 128
ROWS = 8
OFFSET = 8
AHEAD = 6
CUTS = (0, 11, 19, 27)
TINY = 1.1754944e-38


def root(square):
    return square * lax.rsqrt(jnp.maximum(square, TINY))


def kernel(sizes, planes, vel, y_gap, size_out, lm_out, mm_out, coef_out, pad, field, gap, last, gaps, acc, sent, got,
           load_sem, send_sem, recv_sem, sum_send, sum_recv):
    nz, nxl, ny, nxh, nc = sizes
    nx, depth = vel.shape[1], vel.shape[2]
    chunks = vel.shape[3] // LANES
    tiles = depth // ROWS
    me = tuple(lax.axis_index(name) for name in AXES)

    loads = []
    for part in range(3):
        for chunk in range(chunks):
            loads.append(
                pltpu.make_async_copy(
                    vel.at[part, :, :, pl.ds(chunk * LANES, LANES)],
                    pad.at[part, chunk, pl.ds(2, nx), pl.ds(OFFSET, depth), :],
                    load_sem.at[part * chunks + chunk],
                )
            )
    loads.append(pltpu.make_async_copy(y_gap.at[pl.ds(0, chunks * LANES)], gap, load_sem.at[3 * chunks]))
    loads.append(pltpu.make_async_copy(y_gap, last, load_sem.at[3 * chunks + 1]))
    for load in loads:
        load.start()

    def along_x(step):
        ring = nz * nxl
        spot = lax.rem(me[0] * nxl + me[1] + step + ring, ring)
        return (spot // nxl, lax.rem(spot, nxl), me[2], me[3], me[4])

    def along_z(step):
        ring = ny * nxh * nc
        spot = lax.rem((me[2] * nxh + me[3]) * nc + me[4] + step + ring, ring)
        return (me[0], me[1], spot // (nxh * nc), lax.rem(spot // nc, nxh), lax.rem(spot, nc))

    def around(gx_step, gz_step):
        z, xl, *_ = along_x(gx_step)
        return (z, xl, *along_z(gz_step)[2:])

    outer = me[4] == nc - 1

    def shifted(axes, off, sign=1):
        spot = list(me)
        for axis, step in zip(axes, off):
            spot[axis] = lax.rem(me[axis] + sign * step + sizes[axis], sizes[axis])
        return tuple(spot)

    in_plane, in_line = (1, 2, 3), (0, 4)
    plane_offs = list(itertools.product(range(nxl), range(ny), range(nxh)))[1:]
    line_offs = [(step, 0) for step in range(1, nz)] + [(step, 1) for step in range(nz)]
    plane_mine = (me[1] * ny + me[2]) * nxh + me[3]
    members = len(plane_offs) + 1

    barrier = pltpu.get_barrier_semaphore()
    steps = [(1, 0), (-1, 0), (0, 1), (0, -1), (1, 1), (1, -1), (-1, 1), (-1, -1)]
    greeted = [around(*step) for step in steps] + [shifted(in_line, off) for off in line_offs]
    for other in greeted:
        pl.semaphore_signal(barrier, inc=1, device_id=other, device_id_type=MESH)

    for off in plane_offs:
        there = shifted(in_plane, off)
        pl.semaphore_signal(barrier, inc=1, device_id=(*there[:4], 1 - me[4]), device_id_type=MESH)

    @pl.when(outer)
    def _():
        for off in plane_offs:
            pl.semaphore_signal(barrier, inc=1, device_id=shifted(in_plane, off), device_id_type=MESH)

    acc[...] = jnp.zeros_like(acc)
    for load in loads:
        load.wait()
    pl.semaphore_wait(barrier, len(greeted) + jnp.where(outer, 2, 1) * len(plane_offs))

    def rim(number, source, target, other):
        return pltpu.make_async_remote_copy(
            src_ref=pad.at[:, :, pl.ds(*source[0]), pl.ds(*source[1]), :],
            dst_ref=pad.at[:, :, pl.ds(*target[0]), pl.ds(*target[1]), :],
            send_sem=send_sem.at[number],
            recv_sem=recv_sem.at[number],
            device_id=other,
            device_id_type=MESH,
        )

    up, down, right, left = along_x(1), along_x(-1), along_z(1), along_z(-1)
    body = (2, nx)
    first_two, last_two = (OFFSET, 2), (OFFSET + depth - 2, 2)
    before, behind = (OFFSET - 2, 2), (OFFSET + depth, 2)
    sides = [
        rim(0, (body, last_two), (body, before), right),
        rim(1, (body, first_two), (body, behind), left),
    ]
    strips = []
    cuts = [(OFFSET + a, b - a) for a, b in zip(CUTS, CUTS[1:] + (depth,))]
    for number, cut in enumerate(cuts):
        strips.append((
            rim(2 + 2 * number, ((nx, 2), cut), ((0, 2), cut), up),
            rim(3 + 2 * number, ((2, 2), cut), ((nx + 2, 2), cut), down),
        ))
    first = 2 + 2 * len(cuts)
    corners = [
        rim(first, ((nx, 2), last_two), ((0, 2), before), around(1, 1)),
        rim(first + 1, ((nx, 2), first_two), ((0, 2), behind), around(1, -1)),
        rim(first + 2, ((2, 2), last_two), ((nx + 2, 2), before), around(-1, 1)),
        rim(first + 3, ((2, 2), first_two), ((nx + 2, 2), behind), around(-1, -1)),
    ]

    for copy in sides + corners + [strip for pair in strips for strip in pair]:
        copy.start()

    lane = lax.broadcasted_iota(jnp.int32, (ROWS, LANES), 1)
    low, high = lane == 0, lane == LANES - 1
    zero = jnp.zeros((ROWS, LANES), jnp.float32)
    for chunk in range(chunks):
        line = pl.ds(chunk * LANES, LANES)
        here = gap[line].reshape(1, LANES)
        if chunk + 1 < chunks:
            then = gap[pl.ds((chunk + 1) * LANES, LANES)].reshape(1, LANES)
        else:
            then = last[chunks * LANES]
        after = pltpu.roll(jnp.where(low[:1], then, here), LANES - 1, 1)
        span = here + after
        width_sq = jnp.exp((2.0 / 3.0) * jnp.log(0.5 * span))
        gaps[0:1, line] = 2.0 / span
        gaps[1:2, line] = width_sq * (1.0 / 256.0)
        gaps[2:3, line] = width_sq * width_sq * (1.0 / 256.0)
        gaps[3:4, line] = width_sq

    def strains(row, tile):
        at = pl.multiple_of(ROWS * tile, ROWS) + (OFFSET - AHEAD)

        def speed(line, part, chunk, dx=0, dz=0):
            return pad[part, chunk, row + line + 2 + dx, pl.ds(at + dz, ROWS), :]

        lines, parts = range(2), range(3)
        middle = [[[speed(line, part, chunk) for chunk in range(chunks)] for part in parts] for line in lines]
        before = [[[pltpu.roll(v, 1, 1) for v in vs] for vs in rows] for rows in middle]
        after = [[[pltpu.roll(v, LANES - 1, 1) for v in vs] for vs in rows] for rows in middle]
        for line in lines:
            for chunk in range(chunks):
                rate = jnp.broadcast_to(gaps[0:1, pl.ds(chunk * LANES, LANES)], (ROWS, LANES))

                def slope_y(part):
                    above, below = after[line][part], before[line][part]
                    upper = jnp.where(high, above[chunk + 1] if chunk + 1 < chunks else zero, above[chunk])
                    lower = jnp.where(low, below[chunk - 1] if chunk else zero, below[chunk])
                    return (upper - lower) * rate

                def slope_x(part):
                    return speed(line, part, chunk, dx=1) - speed(line, part, chunk, dx=-1)

                def slope_z(part):
                    return speed(line, part, chunk, dz=1) - speed(line, part, chunk, dz=-1)

                strain = [
                    slope_x(0),
                    slope_y(1),
                    slope_z(2),
                    slope_y(0) + slope_x(1),
                    slope_z(0) + slope_x(2),
                    slope_z(1) + slope_y(2),
                ]
                ours = [middle[line][part][chunk] for part in parts]
                square = [s * s for s in strain]
                size = root(0.5 * (square[0] + square[1] + square[2]) + 0.25 * (square[3] + square[4] + square[5]))
                pairs = [ours[0] * ours[0], ours[1] * ours[1], ours[2] * ours[2],
                         ours[0] * ours[1], ours[0] * ours[2], ours[1] * ours[2]]
                values = strain + [size * s for s in strain] + pairs + ours + [size]
                for number, value in enumerate(values):
                    field[number, chunk, row + line + 1, pl.ds(pl.multiple_of(ROWS * tile, ROWS), ROWS), :] = value

    def model(row, tile):
        base = pl.multiple_of(ROWS * tile, ROWS)
        for chunk in range(chunks):
            def smooth(number):
                lines = []
                for k in range(4):
                    a, b, c = (field[number, chunk, row + k, pl.ds(base + AHEAD + dz, ROWS), :] for dz in (-1, 0, 1))
                    lines.append((a + c) + (b + b))
                pair = [lines[k] + lines[k + 1] for k in range(3)]
                return [pair[k] + pair[k + 1] for k in range(2)]

            test = [smooth(k) for k in range(6)]
            speeds = [[0.25 * s for s in smooth(18 + k)] for k in range(3)]
            scale = []
            for k in range(2):
                t = [v[k] * v[k] for v in test]
                scale.append(root((1.0 / 32.0) * (t[0] + t[1] + t[2]) + (1.0 / 64.0) * (t[3] + t[4] + t[5])))
            lm, mm_d, mm_o = [zero, zero], [zero, zero], [zero, zero]
            for number, (i, j) in enumerate(((0, 0), (1, 1), (2, 2), (0, 1), (0, 2), (1, 2))):
                stress, pairs = smooth(6 + number), smooth(12 + number)
                for k in range(2):
                    term = stress[k] - scale[k] * test[number][k]
                    lm[k] = lm[k] + (pairs[k] - speeds[i][k] * speeds[j][k]) * term
                    if number < 3:
                        mm_d[k] = mm_d[k] + term * term
                    else:
                        mm_o[k] = mm_o[k] + term * term
            lm_scale = jnp.broadcast_to(gaps[1:2, pl.ds(chunk * LANES, LANES)], (ROWS, LANES))
            mm_scale = jnp.broadcast_to(gaps[2:3, pl.ds(chunk * LANES, LANES)], (ROWS, LANES))
            lm = [lm_scale * v for v in lm]
            mm = [mm_scale * (a + 0.5 * b) for a, b in zip(mm_d, mm_o)]
            for k in range(2):
                spot = (row + k, pl.ds(base, ROWS), pl.ds(chunk * LANES, LANES))
                size_out[spot] = field[21, chunk, row + k + 1, pl.ds(base + AHEAD, ROWS), :]
                lm_out[spot] = lm[k]
                mm_out[spot] = mm[k]
            acc[chunk] += lm[0] + lm[1]
            acc[chunks + chunk] += mm[0] + mm[1]

    inner, models = tiles, 2 * tiles - 2
    joint = models + tiles

    def step(k, carry):
        second = k > joint + 1
        side = jnp.where(second, 1 - me[1], me[1])
        edge = jnp.logical_and(k >= models, k != joint)
        spot = jnp.where(second, k - joint - 2, jnp.where(k > joint, tiles, k - models))

        @pl.when(k == inner - 1)
        def _():
            sides[0].wait_recv()

        @pl.when(k == joint)
        def _():
            sides[1].wait_recv()

        def landed(number, cut):
            there = pad.at[:, :, pl.ds(side * (nx + 2), 2), pl.ds(*cut), :]
            pltpu.make_async_copy(there, there, recv_sem.at[number]).wait()

        for number, cut in enumerate(cuts):
            @pl.when(jnp.logical_and(edge, spot == (number + 1 if number else 0)))
            def _(number=number, cut=cut):
                if number == 0:
                    landed(first + 2 * side, before)
                landed(2 + 2 * number + side, cut)
                if number == len(cuts) - 1:
                    landed(first + 1 + 2 * side, behind)

        tile = jnp.where(edge, spot, jnp.where(k == joint, tiles, jnp.where(k == inner - 1, 0, k + 1)))
        start = jnp.where(edge, side * nx - 1, 1)
        count = jnp.where(edge, 1, jnp.where(jnp.logical_or(k < inner, k == joint), (nx - 2) // 2, 0))

        def strain_turn(row, carry):
            strains(start + 2 * row, tile)
            return carry
        lax.fori_loop(0, count, strain_turn, 0)

        model_tile = jnp.where(edge, spot - 1, jnp.where(k == joint, tiles - 1, k - inner + 1))
        block = jnp.where(edge, side * (nx - 2), 2)
        turns = jnp.where(edge, jnp.where(spot > 0, 1, 0), jnp.where(k < inner - 1, 0, (nx - 4) // 2))

        def model_turn(turn, carry):
            model(block + 2 * turn, model_tile)
            return carry
        lax.fori_loop(0, turns, model_turn, 0)
        return carry

    lax.fori_loop(0, joint + tiles + 3, step, 0)

    for number in range(2 * chunks):
        sent[0, number : number + 1, :] = jnp.sum(acc[number], axis=0, keepdims=True)
    for number in range(2 * chunks, ROWS):
        sent[0, number : number + 1, :] = jnp.zeros((1, LANES), jnp.float32)
    held = 2 * chunks

    def send(source, slot, number, other):
        pltpu.make_async_remote_copy(
            src_ref=sent.at[source, pl.ds(0, held)], dst_ref=got.at[slot, pl.ds(0, held)],
            send_sem=sum_send.at[0], recv_sem=sum_recv.at[number],
            device_id=other, device_id_type=MESH,
        ).start()

    def arrived(start, count, sem):
        there = got.at[pl.ds(start, count), pl.ds(0, held)]
        pltpu.make_async_copy(there, there, sem).wait()

    def added(terms):
        while len(terms) > 1:
            terms = [a + b for a, b in zip(terms[::2], terms[1::2])]
        return terms[0]

    line_at = 2 * members

    def to_outer(off):
        spot = shifted(in_plane, off)
        return (*spot[:4], nc - 1)

    @pl.when(jnp.logical_not(outer))
    def _():
        for off in [(0, 0, 0)] + plane_offs:
            send(0, plane_mine, 1, to_outer(off))
        arrived(0, members, sum_send.at[0])
        arrived(line_at, nz, sum_recv.at[2])

    @pl.when(outer)
    def _():
        for off in plane_offs:
            send(0, members + plane_mine, 1, shifted(in_plane, off))
        got[members + plane_mine] = sent[0]
        arrived(0, 2 * members - 1, sum_recv.at[1])
        whole = added([got[k] for k in range(2 * members)])
        sent[1] = whole
        for off in line_offs:
            send(1, line_at + me[0], 2, shifted(in_line, off))
        got[line_at + me[0]] = whole
        arrived(line_at, nz - 1, sum_recv.at[2])
        arrived(0, members - 1, sum_send.at[0])
        arrived(0, len(line_offs), sum_send.at[0])

    total = added([got[line_at + k] for k in range(nz)])

    for chunk in range(chunks):
        line = pl.ds(chunk * LANES, LANES)
        share = total[chunk : chunk + 1, :] * (1.0 / planes)
        below = total[chunks + chunk : chunks + chunk + 1, :] * (1.0 / planes) + 1e-06
        coefficient = share / below
        coef_out[0:1, line] = coefficient
        coef_out[1:2, line] = coefficient * gaps[3:4, line]
    for copy in sides + corners + [strip for pair in strips for strip in pair]:
        copy.wait_send()


def finish(size, lm, mm, coef, eddy_out, lm_out, mm_out, coef_out, eddy, sem):
    copies = [
        pltpu.make_async_copy(lm, lm_out, sem.at[0]),
        pltpu.make_async_copy(mm, mm_out, sem.at[1]),
        pltpu.make_async_copy(coef.at[0], coef_out, sem.at[2]),
        pltpu.make_async_copy(eddy, eddy_out, sem.at[3]),
    ]
    for copy in copies[:3]:
        copy.start()
    eddy[...] = size[...] * coef[1:2, :].reshape(1, 1, coef.shape[1])
    copies[3].start()
    for copy in copies:
        copy.wait()


def solution(mesh):
    shape = (8, 2, 4, 2, 2)
    torus = Mesh(mesh.devices.reshape(shape), AXES)

    def per_device(velocity, y_gap):
        _, nx, depth, height = velocity.shape
        chunks, tiles = height // LANES, depth // ROWS
        cells = nx * lax.axis_size(GX) * depth * lax.axis_size(GZ)
        rims = 2 + 2 * len(CUTS) + 4
        ways = 2 * shape[1] * shape[2] * shape[3] + shape[0]
        grid = jax.ShapeDtypeStruct((nx, depth, height), jnp.float32)
        vmem = pl.BlockSpec(memory_space=pltpu.VMEM)
        hbm = pl.BlockSpec(memory_space=pltpu.HBM)
        size, lm, mm, coefficient = pl.pallas_call(
            lambda *refs: kernel(shape, cells, *refs),
            out_shape=(grid, grid, grid, jax.ShapeDtypeStruct((2, height), jnp.float32)),
            in_specs=[hbm, hbm],
            out_specs=(vmem, vmem, vmem, vmem),
            scratch_shapes=[
                pltpu.VMEM((3, chunks, nx + 4, depth + 16, LANES), jnp.float32),
                pltpu.VMEM((22, chunks, nx + 2, depth + 8, LANES), jnp.float32),
                pltpu.VMEM((height,), jnp.float32),
                pltpu.SMEM((height + 1,), jnp.float32),
                pltpu.VMEM((4, height), jnp.float32),
                pltpu.VMEM((2 * chunks, ROWS, LANES), jnp.float32),
                pltpu.VMEM((2, ROWS, LANES), jnp.float32),
                pltpu.VMEM((ways, ROWS, LANES), jnp.float32),
                pltpu.SemaphoreType.DMA((3 * chunks + 2,)),
                pltpu.SemaphoreType.DMA((rims,)),
                pltpu.SemaphoreType.DMA((rims,)),
                pltpu.SemaphoreType.DMA((1,)),
                pltpu.SemaphoreType.DMA((3,)),
            ],
            compiler_params=pltpu.CompilerParams(
                collective_id=0, has_side_effects=True, vmem_limit_bytes=40 * 1024 * 1024
            ),
            name="smagorinsky",
        )(pltpu.with_memory_space_constraint(velocity, pltpu.HBM), pltpu.with_memory_space_constraint(y_gap, pltpu.HBM))
        return pl.pallas_call(
            finish,
            out_shape=(grid, grid, grid, jax.ShapeDtypeStruct((height,), jnp.float32)),
            in_specs=[vmem] * 4,
            out_specs=[hbm] * 4,
            scratch_shapes=[pltpu.VMEM((nx, depth, height), jnp.float32), pltpu.SemaphoreType.DMA((4,))],
            compiler_params=pltpu.CompilerParams(vmem_limit_bytes=4 * 1024 * 1024),
            name="finish",
        )(size, lm, mm, coefficient)

    return jax.shard_map(
        per_device,
        mesh=torus,
        in_specs=(P(None, GX, GZ, None), P()),
        out_specs=(P(GX, GZ, None), P(GX, GZ, None), P(GX, GZ, None), P()),
        check_vma=False,
    )
```

```python
import itertools

import jax
import jax.numpy as jnp
from jax import lax
from jax.experimental import pallas as pl
from jax.experimental.pallas import tpu as pltpu
from jax.sharding import Mesh
from jax.sharding import PartitionSpec as P

AXES = ("gx_0", "gx_1", "gz_0", "gz_1", "gz_2")
GX = ("gx_0", "gx_1")
GZ = ("gz_0", "gz_1", "gz_2")
MESH = pl.DeviceIdType.MESH

LANES = 128
ROWS = 8
OFFSET = 8
AHEAD = 6
CUTS = ((30, 2), (0, 11), (11, 8), (19, 8), (27, 3))
TINY = 1.1754944e-38


def root(square):
    return square * lax.rsqrt(jnp.maximum(square, TINY))


def kernel(sizes, planes, vel, y_gap, size_out, lm_out, mm_out, coef_out, pad, field, gap, last, gaps, acc, sent, got,
           load_sem, send_sem, recv_sem, sum_send, sum_recv):
    nz, nxl, ny, nxh, nc = sizes
    nx, depth = vel.shape[1], vel.shape[2]
    chunks = vel.shape[3] // LANES
    tiles = depth // ROWS
    me = tuple(lax.axis_index(name) for name in AXES)

    loads = []
    for part in range(3):
        for chunk in range(chunks):
            loads.append(
                pltpu.make_async_copy(
                    vel.at[part, :, :, pl.ds(chunk * LANES, LANES)],
                    pad.at[part, chunk, pl.ds(2, nx), pl.ds(OFFSET, depth), :],
                    load_sem.at[part * chunks + chunk],
                )
            )
    loads.append(pltpu.make_async_copy(y_gap.at[pl.ds(0, chunks * LANES)], gap, load_sem.at[3 * chunks]))
    loads.append(pltpu.make_async_copy(y_gap, last, load_sem.at[3 * chunks + 1]))
    for load in loads:
        load.start()

    def along_x(step):
        ring = nz * nxl
        spot = lax.rem(me[0] * nxl + me[1] + step + ring, ring)
        return (spot // nxl, lax.rem(spot, nxl), me[2], me[3], me[4])

    def along_z(step):
        ring = ny * nxh * nc
        spot = lax.rem((me[2] * nxh + me[3]) * nc + me[4] + step + ring, ring)
        return (me[0], me[1], spot // (nxh * nc), lax.rem(spot // nc, nxh), lax.rem(spot, nc))

    def around(gx_step, gz_step):
        z, xl, *_ = along_x(gx_step)
        return (z, xl, *along_z(gz_step)[2:])

    outer = me[4] == nc - 1

    def shifted(axes, off, sign=1):
        spot = list(me)
        for axis, step in zip(axes, off):
            spot[axis] = lax.rem(me[axis] + sign * step + sizes[axis], sizes[axis])
        return tuple(spot)

    in_plane, in_line = (1, 2, 3), (0, 4)
    plane_offs = list(itertools.product(range(nxl), range(ny), range(nxh)))[1:]
    line_offs = [(step, 0) for step in range(1, nz)] + [(step, 1) for step in range(nz)]
    plane_mine = (me[1] * ny + me[2]) * nxh + me[3]
    members = len(plane_offs) + 1

    barrier = pltpu.get_barrier_semaphore()
    beyond = 2 * me[4] - 1
    steps = [(1, 0), (-1, 0), (0, 1), (0, -1), (1, beyond), (-1, beyond)]
    greeted = [around(*step) for step in steps] + [shifted(in_line, off) for off in line_offs]
    for other in greeted:
        pl.semaphore_signal(barrier, inc=1, device_id=other, device_id_type=MESH)

    for off in plane_offs:
        there = shifted(in_plane, off)
        pl.semaphore_signal(barrier, inc=1, device_id=(*there[:4], 1 - me[4]), device_id_type=MESH)

    @pl.when(outer)
    def _():
        for off in plane_offs:
            pl.semaphore_signal(barrier, inc=1, device_id=shifted(in_plane, off), device_id_type=MESH)

    acc[...] = jnp.zeros_like(acc)
    for load in loads:
        load.wait()
    pl.semaphore_wait(barrier, len(greeted) + jnp.where(outer, 2, 1) * len(plane_offs))

    def rim(number, source, target, other):
        return pltpu.make_async_remote_copy(
            src_ref=pad.at[:, :, pl.ds(*source[0]), pl.ds(*source[1]), :],
            dst_ref=pad.at[:, :, pl.ds(*target[0]), pl.ds(*target[1]), :],
            send_sem=send_sem.at[number],
            recv_sem=recv_sem.at[number],
            device_id=other,
            device_id_type=MESH,
        )

    up, down, right, left = along_x(1), along_x(-1), along_z(1), along_z(-1)
    body = (2, nx)
    first_two, last_two = (OFFSET, 2), (OFFSET + depth - 2, 2)
    before, behind = (OFFSET - 2, 2), (OFFSET + depth, 2)
    sides = [
        rim(0, (body, last_two), (body, before), right),
        rim(1, (body, first_two), (body, behind), left),
    ]
    strips = []
    cuts = [(OFFSET + at, count) for at, count in CUTS]
    for number, cut in enumerate(cuts):
        strips.append((
            rim(2 + 2 * number, ((nx, 2), cut), ((0, 2), cut), up),
            rim(3 + 2 * number, ((2, 2), cut), ((nx + 2, 2), cut), down),
        ))
    first = 2 + 2 * len(cuts)
    own = jnp.where(outer, last_two[0], first_two[0]), 2
    far = jnp.where(outer, before[0], behind[0]), 2
    handed = jnp.where(outer, first_two[0], last_two[0]), 2
    taken = jnp.where(outer, behind[0], before[0]), 2
    corners = [
        rim(first + 1 - me[4], ((nx, 2), own), ((0, 2), far), around(1, beyond)),
        rim(first + 3 - me[4], ((2, 2), own), ((nx + 2, 2), far), around(-1, beyond)),
    ]

    def hand(side):
        rows = (side * (nx + 2), 2)
        return rim(first + 2 * side + me[4], (rows, handed), (rows, taken), (*me[:4], nc - 1 - me[4]))

    for copy in sides + corners:
        copy.start()

    lane = lax.broadcasted_iota(jnp.int32, (ROWS, LANES), 1)
    low, high = lane == 0, lane == LANES - 1
    zero = jnp.zeros((ROWS, LANES), jnp.float32)
    for chunk in range(chunks):
        line = pl.ds(chunk * LANES, LANES)
        here = gap[line].reshape(1, LANES)
        if chunk + 1 < chunks:
            then = gap[pl.ds((chunk + 1) * LANES, LANES)].reshape(1, LANES)
        else:
            then = last[chunks * LANES]
        after = pltpu.roll(jnp.where(low[:1], then, here), LANES - 1, 1)
        span = here + after
        width_sq = jnp.exp((2.0 / 3.0) * jnp.log(0.5 * span))
        gaps[0:1, line] = 2.0 / span
        gaps[1:2, line] = width_sq * (1.0 / 256.0)
        gaps[2:3, line] = width_sq * width_sq * (1.0 / 256.0)
        gaps[3:4, line] = width_sq

    def strains(row, tile):
        at = pl.multiple_of(ROWS * tile, ROWS) + (OFFSET - AHEAD)

        def speed(line, part, chunk, dx=0, dz=0):
            return pad[part, chunk, row + line + 2 + dx, pl.ds(at + dz, ROWS), :]

        lines, parts = range(2), range(3)
        middle = [[[speed(line, part, chunk) for chunk in range(chunks)] for part in parts] for line in lines]
        before = [[[pltpu.roll(v, 1, 1) for v in vs] for vs in rows] for rows in middle]
        after = [[[pltpu.roll(v, LANES - 1, 1) for v in vs] for vs in rows] for rows in middle]
        for line in lines:
            for chunk in range(chunks):
                rate = jnp.broadcast_to(gaps[0:1, pl.ds(chunk * LANES, LANES)], (ROWS, LANES))

                def slope_y(part):
                    above, below = after[line][part], before[line][part]
                    upper = jnp.where(high, above[chunk + 1] if chunk + 1 < chunks else zero, above[chunk])
                    lower = jnp.where(low, below[chunk - 1] if chunk else zero, below[chunk])
                    return (upper - lower) * rate

                def slope_x(part):
                    return speed(line, part, chunk, dx=1) - speed(line, part, chunk, dx=-1)

                def slope_z(part):
                    return speed(line, part, chunk, dz=1) - speed(line, part, chunk, dz=-1)

                strain = [
                    slope_x(0),
                    slope_y(1),
                    slope_z(2),
                    slope_y(0) + slope_x(1),
                    slope_z(0) + slope_x(2),
                    slope_z(1) + slope_y(2),
                ]
                ours = [middle[line][part][chunk] for part in parts]
                square = [s * s for s in strain]
                size = root(0.5 * (square[0] + square[1] + square[2]) + 0.25 * (square[3] + square[4] + square[5]))
                pairs = [ours[0] * ours[0], ours[1] * ours[1], ours[2] * ours[2],
                         ours[0] * ours[1], ours[0] * ours[2], ours[1] * ours[2]]
                values = strain + [size * s for s in strain] + pairs + ours + [size]
                for number, value in enumerate(values):
                    field[number, chunk, row + line + 1, pl.ds(pl.multiple_of(ROWS * tile, ROWS), ROWS), :] = value

    def model(row, tile):
        base = pl.multiple_of(ROWS * tile, ROWS)
        for chunk in range(chunks):
            def smooth(number):
                lines = []
                for k in range(4):
                    a, b, c = (field[number, chunk, row + k, pl.ds(base + AHEAD + dz, ROWS), :] for dz in (-1, 0, 1))
                    lines.append((a + c) + (b + b))
                pair = [lines[k] + lines[k + 1] for k in range(3)]
                return [pair[k] + pair[k + 1] for k in range(2)]

            test = [smooth(k) for k in range(6)]
            speeds = [[0.25 * s for s in smooth(18 + k)] for k in range(3)]
            scale = []
            for k in range(2):
                t = [v[k] * v[k] for v in test]
                scale.append(root((1.0 / 32.0) * (t[0] + t[1] + t[2]) + (1.0 / 64.0) * (t[3] + t[4] + t[5])))
            lm, mm_d, mm_o = [zero, zero], [zero, zero], [zero, zero]
            for number, (i, j) in enumerate(((0, 0), (1, 1), (2, 2), (0, 1), (0, 2), (1, 2))):
                stress, pairs = smooth(6 + number), smooth(12 + number)
                for k in range(2):
                    term = stress[k] - scale[k] * test[number][k]
                    lm[k] = lm[k] + (pairs[k] - speeds[i][k] * speeds[j][k]) * term
                    if number < 3:
                        mm_d[k] = mm_d[k] + term * term
                    else:
                        mm_o[k] = mm_o[k] + term * term
            lm_scale = jnp.broadcast_to(gaps[1:2, pl.ds(chunk * LANES, LANES)], (ROWS, LANES))
            mm_scale = jnp.broadcast_to(gaps[2:3, pl.ds(chunk * LANES, LANES)], (ROWS, LANES))
            lm = [lm_scale * v for v in lm]
            mm = [mm_scale * (a + 0.5 * b) for a, b in zip(mm_d, mm_o)]
            for k in range(2):
                spot = (row + k, pl.ds(base, ROWS), pl.ds(chunk * LANES, LANES))
                size_out[spot] = field[21, chunk, row + k + 1, pl.ds(base + AHEAD, ROWS), :]
                lm_out[spot] = lm[k]
                mm_out[spot] = mm[k]
            acc[chunk] += lm[0] + lm[1]
            acc[chunks + chunk] += mm[0] + mm[1]

    inner, models = tiles, 2 * tiles - 2
    joint = models + tiles

    def step(k, carry):
        second = k > joint + 1
        side = jnp.where(second, 1 - me[1], me[1])
        edge = jnp.logical_and(k >= models, k != joint)
        spot = jnp.where(second, k - joint - 2, jnp.where(k > joint, tiles, k - models))

        @pl.when(k == 1)
        def _():
            for copy in sides:
                copy.wait_send()
            for pair in strips:
                for copy in pair:
                    copy.start()

        @pl.when(k == inner - 1)
        def _():
            sides[0].wait_recv()

        @pl.when(k == joint)
        def _():
            sides[1].wait_recv()

        def landed(number, cut):
            there = pad.at[:, :, pl.ds(side * (nx + 2), 2), pl.ds(*cut), :]
            pltpu.make_async_copy(there, there, recv_sem.at[number]).wait()

        def strip(number):
            landed(2 + 2 * number + side, cuts[number])

        @pl.when(jnp.logical_and(edge, spot == 0))
        def _():
            strip(0)

            @pl.when(jnp.logical_not(outer))
            def _():
                hand(side).start()

            strip(1)

            @pl.when(outer)
            def _():
                hand(side).start()

            landed(first + 2 * side, before)

        for number in range(2, len(cuts)):
            @pl.when(jnp.logical_and(edge, spot == number))
            def _(number=number):
                strip(number)
                if number == len(cuts) - 1:
                    landed(first + 1 + 2 * side, behind)

        tile = jnp.where(edge, spot, jnp.where(k == joint, tiles, jnp.where(k == inner - 1, 0, k + 1)))
        start = jnp.where(edge, side * nx - 1, 1)
        count = jnp.where(edge, 1, jnp.where(jnp.logical_or(k < inner, k == joint), (nx - 2) // 2, 0))

        def strain_turn(row, carry):
            strains(start + 2 * row, tile)
            return carry
        lax.fori_loop(0, count, strain_turn, 0)

        model_tile = jnp.where(edge, spot - 1, jnp.where(k == joint, tiles - 1, k - inner + 1))
        block = jnp.where(edge, side * (nx - 2), 2)
        turns = jnp.where(edge, jnp.where(spot > 0, 1, 0), jnp.where(k < inner - 1, 0, (nx - 4) // 2))

        def model_turn(turn, carry):
            model(block + 2 * turn, model_tile)
            return carry
        lax.fori_loop(0, turns, model_turn, 0)
        return carry

    lax.fori_loop(0, joint + tiles + 3, step, 0)

    for number in range(2 * chunks):
        sent[0, number : number + 1, :] = jnp.sum(acc[number], axis=0, keepdims=True)
    for number in range(2 * chunks, ROWS):
        sent[0, number : number + 1, :] = jnp.zeros((1, LANES), jnp.float32)
    held = 2 * chunks

    def send(source, slot, number, other):
        pltpu.make_async_remote_copy(
            src_ref=sent.at[source, pl.ds(0, held)], dst_ref=got.at[slot, pl.ds(0, held)],
            send_sem=sum_send.at[0], recv_sem=sum_recv.at[number],
            device_id=other, device_id_type=MESH,
        ).start()

    def arrived(start, count, sem):
        there = got.at[pl.ds(start, count), pl.ds(0, held)]
        pltpu.make_async_copy(there, there, sem).wait()

    def added(terms):
        while len(terms) > 1:
            terms = [a + b for a, b in zip(terms[::2], terms[1::2])]
        return terms[0]

    line_at = 2 * members

    def to_outer(off):
        spot = shifted(in_plane, off)
        return (*spot[:4], nc - 1)

    @pl.when(jnp.logical_not(outer))
    def _():
        for off in [(0, 0, 0)] + plane_offs:
            send(0, plane_mine, 1, to_outer(off))
        arrived(0, members, sum_send.at[0])
        arrived(line_at, nz, sum_recv.at[2])

    @pl.when(outer)
    def _():
        for off in plane_offs:
            send(0, members + plane_mine, 1, shifted(in_plane, off))
        got[members + plane_mine] = sent[0]
        arrived(0, 2 * members - 1, sum_recv.at[1])
        whole = added([got[k] for k in range(2 * members)])
        sent[1] = whole
        for off in line_offs:
            send(1, line_at + me[0], 2, shifted(in_line, off))
        got[line_at + me[0]] = whole
        arrived(line_at, nz - 1, sum_recv.at[2])
        arrived(0, members - 1, sum_send.at[0])
        arrived(0, len(line_offs), sum_send.at[0])

    total = added([got[line_at + k] for k in range(nz)])

    for chunk in range(chunks):
        line = pl.ds(chunk * LANES, LANES)
        share = total[chunk : chunk + 1, :] * (1.0 / planes)
        below = total[chunks + chunk : chunks + chunk + 1, :] * (1.0 / planes) + 1e-06
        coefficient = share / below
        coef_out[0:1, line] = coefficient
        coef_out[1:2, line] = coefficient * gaps[3:4, line]
    for copy in corners + [hand(0), hand(1)] + [strip for pair in strips for strip in pair]:
        copy.wait_send()


def finish(size, lm, mm, coef, eddy_out, lm_out, mm_out, coef_out, eddy, sem):
    copies = [
        pltpu.make_async_copy(lm, lm_out, sem.at[0]),
        pltpu.make_async_copy(mm, mm_out, sem.at[1]),
        pltpu.make_async_copy(coef.at[0], coef_out, sem.at[2]),
        pltpu.make_async_copy(eddy, eddy_out, sem.at[3]),
    ]
    for copy in copies[:3]:
        copy.start()
    eddy[...] = size[...] * coef[1:2, :].reshape(1, 1, coef.shape[1])
    copies[3].start()
    for copy in copies:
        copy.wait()


def solution(mesh):
    shape = (8, 2, 4, 2, 2)
    torus = Mesh(mesh.devices.reshape(shape), AXES)

    def per_device(velocity, y_gap):
        _, nx, depth, height = velocity.shape
        chunks, tiles = height // LANES, depth // ROWS
        cells = nx * lax.axis_size(GX) * depth * lax.axis_size(GZ)
        rims = 2 + 2 * len(CUTS) + 4
        ways = 2 * shape[1] * shape[2] * shape[3] + shape[0]
        grid = jax.ShapeDtypeStruct((nx, depth, height), jnp.float32)
        vmem = pl.BlockSpec(memory_space=pltpu.VMEM)
        hbm = pl.BlockSpec(memory_space=pltpu.HBM)
        size, lm, mm, coefficient = pl.pallas_call(
            lambda *refs: kernel(shape, cells, *refs),
            out_shape=(grid, grid, grid, jax.ShapeDtypeStruct((2, height), jnp.float32)),
            in_specs=[hbm, hbm],
            out_specs=(vmem, vmem, vmem, vmem),
            scratch_shapes=[
                pltpu.VMEM((3, chunks, nx + 4, depth + 16, LANES), jnp.float32),
                pltpu.VMEM((22, chunks, nx + 2, depth + 8, LANES), jnp.float32),
                pltpu.VMEM((height,), jnp.float32),
                pltpu.SMEM((height + 1,), jnp.float32),
                pltpu.VMEM((4, height), jnp.float32),
                pltpu.VMEM((2 * chunks, ROWS, LANES), jnp.float32),
                pltpu.VMEM((2, ROWS, LANES), jnp.float32),
                pltpu.VMEM((ways, ROWS, LANES), jnp.float32),
                pltpu.SemaphoreType.DMA((3 * chunks + 2,)),
                pltpu.SemaphoreType.DMA((rims,)),
                pltpu.SemaphoreType.DMA((rims,)),
                pltpu.SemaphoreType.DMA((1,)),
                pltpu.SemaphoreType.DMA((3,)),
            ],
            compiler_params=pltpu.CompilerParams(
                collective_id=0, has_side_effects=True, vmem_limit_bytes=40 * 1024 * 1024
            ),
            name="smagorinsky",
        )(pltpu.with_memory_space_constraint(velocity, pltpu.HBM), pltpu.with_memory_space_constraint(y_gap, pltpu.HBM))
        return pl.pallas_call(
            finish,
            out_shape=(grid, grid, grid, jax.ShapeDtypeStruct((height,), jnp.float32)),
            in_specs=[vmem] * 4,
            out_specs=[hbm] * 4,
            scratch_shapes=[pltpu.VMEM((nx, depth, height), jnp.float32), pltpu.SemaphoreType.DMA((4,))],
            compiler_params=pltpu.CompilerParams(vmem_limit_bytes=4 * 1024 * 1024),
            name="finish",
        )(size, lm, mm, coefficient)

    return jax.shard_map(
        per_device,
        mesh=torus,
        in_specs=(P(None, GX, GZ, None), P()),
        out_specs=(P(GX, GZ, None), P(GX, GZ, None), P(GX, GZ, None), P()),
        check_vma=False,
    )
```

```python
import itertools

import jax
import jax.numpy as jnp
from jax import lax
from jax.experimental import pallas as pl
from jax.experimental.pallas import tpu as pltpu
from jax.sharding import Mesh
from jax.sharding import PartitionSpec as P

AXES = ("gx_0", "gx_1", "gz_0", "gz_1", "gz_2")
GX = ("gx_0", "gx_1")
GZ = ("gz_0", "gz_1", "gz_2")
MESH = pl.DeviceIdType.MESH

LANES = 128
ROWS = 8
OFFSET = 8
AHEAD = 6
CUTS = ((30, 2), (0, 11), (11, 8), (19, 8), (27, 3))
TINY = 1.1754944e-38


def root(square):
    return square * lax.rsqrt(jnp.maximum(square, TINY))


def kernel(sizes, planes, vel, y_gap, size_out, lm_out, mm_out, coef_out, pad, field, gap, last, gaps, acc, sent, got,
           load_sem, send_sem, recv_sem, sum_send, sum_recv):
    nz, nxl, ny, nxh, nc = sizes
    nx, depth = vel.shape[1], vel.shape[2]
    chunks = vel.shape[3] // LANES
    tiles = depth // ROWS
    me = tuple(lax.axis_index(name) for name in AXES)

    loads = []
    for part in range(3):
        for chunk in range(chunks):
            loads.append(
                pltpu.make_async_copy(
                    vel.at[part, :, :, pl.ds(chunk * LANES, LANES)],
                    pad.at[part, chunk, pl.ds(2, nx), pl.ds(OFFSET, depth), :],
                    load_sem.at[part * chunks + chunk],
                )
            )
    loads.append(pltpu.make_async_copy(y_gap.at[pl.ds(0, chunks * LANES)], gap, load_sem.at[3 * chunks]))
    loads.append(pltpu.make_async_copy(y_gap, last, load_sem.at[3 * chunks + 1]))
    for load in loads:
        load.start()

    def along_x(step):
        ring = nz * nxl
        spot = lax.rem(me[0] * nxl + me[1] + step + ring, ring)
        return (spot // nxl, lax.rem(spot, nxl), me[2], me[3], me[4])

    def along_z(step):
        ring = ny * nxh * nc
        spot = lax.rem((me[2] * nxh + me[3]) * nc + me[4] + step + ring, ring)
        return (me[0], me[1], spot // (nxh * nc), lax.rem(spot // nc, nxh), lax.rem(spot, nc))

    def around(gx_step, gz_step):
        z, xl, *_ = along_x(gx_step)
        return (z, xl, *along_z(gz_step)[2:])

    outer = me[4] == nc - 1

    def shifted(axes, off, sign=1):
        spot = list(me)
        for axis, step in zip(axes, off):
            spot[axis] = lax.rem(me[axis] + sign * step + sizes[axis], sizes[axis])
        return tuple(spot)

    in_plane, in_line = (1, 2, 3), (0, 4)
    def hops(off):
        xl, y, xh = off
        return min(y, ny - y) + (2 * xh if xl == 0 else 1)

    plane_offs = sorted(list(itertools.product(range(nxl), range(ny), range(nxh)))[1:], key=hops, reverse=True)
    line_offs = sorted(list(itertools.product(range(nz), range(nc)))[1:], key=lambda off: -min(off[0], nz - off[0]))
    plane_mine = (me[1] * ny + me[2]) * nxh + me[3]
    members = len(plane_offs) + 1

    barrier = pltpu.get_barrier_semaphore()
    beyond = 2 * me[4] - 1
    steps = [(1, 0), (-1, 0), (0, 1), (0, -1), (1, beyond), (-1, beyond)]
    greeted = [around(*step) for step in steps] + [shifted(in_line, off) for off in line_offs]
    for other in greeted:
        pl.semaphore_signal(barrier, inc=1, device_id=other, device_id_type=MESH)

    for off in plane_offs:
        there = shifted(in_plane, off)
        pl.semaphore_signal(barrier, inc=1, device_id=(*there[:4], 1 - me[4]), device_id_type=MESH)

    @pl.when(outer)
    def _():
        for off in plane_offs:
            pl.semaphore_signal(barrier, inc=1, device_id=shifted(in_plane, off), device_id_type=MESH)

    acc[...] = jnp.zeros_like(acc)
    for load in loads:
        load.wait()
    pl.semaphore_wait(barrier, len(greeted) + jnp.where(outer, 2, 1) * len(plane_offs))

    def rim(number, source, target, other):
        return pltpu.make_async_remote_copy(
            src_ref=pad.at[:, :, pl.ds(*source[0]), pl.ds(*source[1]), :],
            dst_ref=pad.at[:, :, pl.ds(*target[0]), pl.ds(*target[1]), :],
            send_sem=send_sem.at[number],
            recv_sem=recv_sem.at[number],
            device_id=other,
            device_id_type=MESH,
        )

    up, down, right, left = along_x(1), along_x(-1), along_z(1), along_z(-1)
    body = (2, nx)
    first_two, last_two = (OFFSET, 2), (OFFSET + depth - 2, 2)
    before, behind = (OFFSET - 2, 2), (OFFSET + depth, 2)
    sides = [
        rim(0, (body, last_two), (body, before), right),
        rim(1, (body, first_two), (body, behind), left),
    ]
    strips = []
    cuts = [(OFFSET + at, count) for at, count in CUTS]
    for number, cut in enumerate(cuts):
        strips.append((
            rim(2 + 2 * number, ((nx, 2), cut), ((0, 2), cut), up),
            rim(3 + 2 * number, ((2, 2), cut), ((nx + 2, 2), cut), down),
        ))
    first = 2 + 2 * len(cuts)
    own = jnp.where(outer, last_two[0], first_two[0]), 2
    far = jnp.where(outer, before[0], behind[0]), 2
    handed = jnp.where(outer, first_two[0], last_two[0]), 2
    taken = jnp.where(outer, behind[0], before[0]), 2
    corners = [
        rim(first + 1 - me[4], ((nx, 2), own), ((0, 2), far), around(1, beyond)),
        rim(first + 3 - me[4], ((2, 2), own), ((nx + 2, 2), far), around(-1, beyond)),
    ]

    def hand(side):
        rows = (side * (nx + 2), 2)
        return rim(first + 2 * side + me[4], (rows, handed), (rows, taken), (*me[:4], nc - 1 - me[4]))

    for copy in sides + corners:
        copy.start()

    lane = lax.broadcasted_iota(jnp.int32, (ROWS, LANES), 1)
    low, high = lane == 0, lane == LANES - 1
    zero = jnp.zeros((ROWS, LANES), jnp.float32)
    for chunk in range(chunks):
        line = pl.ds(chunk * LANES, LANES)
        here = gap[line].reshape(1, LANES)
        if chunk + 1 < chunks:
            then = gap[pl.ds((chunk + 1) * LANES, LANES)].reshape(1, LANES)
        else:
            then = last[chunks * LANES]
        after = pltpu.roll(jnp.where(low[:1], then, here), LANES - 1, 1)
        span = here + after
        width_sq = jnp.exp((2.0 / 3.0) * jnp.log(0.5 * span))
        gaps[0:1, line] = 2.0 / span
        gaps[1:2, line] = width_sq * (1.0 / 256.0)
        gaps[2:3, line] = width_sq * width_sq * (1.0 / 256.0)
        gaps[3:4, line] = width_sq

    def strains(row, tile):
        at = pl.multiple_of(ROWS * tile, ROWS) + (OFFSET - AHEAD)

        def speed(line, part, chunk, dx=0, dz=0):
            return pad[part, chunk, row + line + 2 + dx, pl.ds(at + dz, ROWS), :]

        lines, parts = range(2), range(3)
        middle = [[[speed(line, part, chunk) for chunk in range(chunks)] for part in parts] for line in lines]
        before = [[[pltpu.roll(v, 1, 1) for v in vs] for vs in rows] for rows in middle]
        after = [[[pltpu.roll(v, LANES - 1, 1) for v in vs] for vs in rows] for rows in middle]
        for line in lines:
            for chunk in range(chunks):
                rate = jnp.broadcast_to(gaps[0:1, pl.ds(chunk * LANES, LANES)], (ROWS, LANES))

                def slope_y(part):
                    above, below = after[line][part], before[line][part]
                    upper = jnp.where(high, above[chunk + 1] if chunk + 1 < chunks else zero, above[chunk])
                    lower = jnp.where(low, below[chunk - 1] if chunk else zero, below[chunk])
                    return (upper - lower) * rate

                def slope_x(part):
                    return speed(line, part, chunk, dx=1) - speed(line, part, chunk, dx=-1)

                def slope_z(part):
                    return speed(line, part, chunk, dz=1) - speed(line, part, chunk, dz=-1)

                strain = [
                    slope_x(0),
                    slope_y(1),
                    slope_z(2),
                    slope_y(0) + slope_x(1),
                    slope_z(0) + slope_x(2),
                    slope_z(1) + slope_y(2),
                ]
                ours = [middle[line][part][chunk] for part in parts]
                square = [s * s for s in strain]
                size = root(0.5 * (square[0] + square[1] + square[2]) + 0.25 * (square[3] + square[4] + square[5]))
                pairs = [ours[0] * ours[0], ours[1] * ours[1], ours[2] * ours[2],
                         ours[0] * ours[1], ours[0] * ours[2], ours[1] * ours[2]]
                values = strain + [size * s for s in strain] + pairs + ours + [size]
                for number, value in enumerate(values):
                    field[number, chunk, row + line + 1, pl.ds(pl.multiple_of(ROWS * tile, ROWS), ROWS), :] = value

    def model(row, tile):
        base = pl.multiple_of(ROWS * tile, ROWS)
        for chunk in range(chunks):
            def smooth(number):
                lines = []
                for k in range(4):
                    a, b, c = (field[number, chunk, row + k, pl.ds(base + AHEAD + dz, ROWS), :] for dz in (-1, 0, 1))
                    lines.append((a + c) + (b + b))
                pair = [lines[k] + lines[k + 1] for k in range(3)]
                return [pair[k] + pair[k + 1] for k in range(2)]

            test = [smooth(k) for k in range(6)]
            speeds = [[0.25 * s for s in smooth(18 + k)] for k in range(3)]
            scale = []
            for k in range(2):
                t = [v[k] * v[k] for v in test]
                scale.append(root((1.0 / 32.0) * (t[0] + t[1] + t[2]) + (1.0 / 64.0) * (t[3] + t[4] + t[5])))
            lm, mm_d, mm_o = [zero, zero], [zero, zero], [zero, zero]
            for number, (i, j) in enumerate(((0, 0), (1, 1), (2, 2), (0, 1), (0, 2), (1, 2))):
                stress, pairs = smooth(6 + number), smooth(12 + number)
                for k in range(2):
                    term = stress[k] - scale[k] * test[number][k]
                    lm[k] = lm[k] + (pairs[k] - speeds[i][k] * speeds[j][k]) * term
                    if number < 3:
                        mm_d[k] = mm_d[k] + term * term
                    else:
                        mm_o[k] = mm_o[k] + term * term
            lm_scale = jnp.broadcast_to(gaps[1:2, pl.ds(chunk * LANES, LANES)], (ROWS, LANES))
            mm_scale = jnp.broadcast_to(gaps[2:3, pl.ds(chunk * LANES, LANES)], (ROWS, LANES))
            lm = [lm_scale * v for v in lm]
            mm = [mm_scale * (a + 0.5 * b) for a, b in zip(mm_d, mm_o)]
            for k in range(2):
                spot = (row + k, pl.ds(base, ROWS), pl.ds(chunk * LANES, LANES))
                size_out[spot] = field[21, chunk, row + k + 1, pl.ds(base + AHEAD, ROWS), :]
                lm_out[spot] = lm[k]
                mm_out[spot] = mm[k]
            acc[chunk] += lm[0] + lm[1]
            acc[chunks + chunk] += mm[0] + mm[1]

    inner, models = tiles, 2 * tiles - 2
    joint = models + tiles

    def step(k, carry):
        second = k > joint + 1
        side = jnp.where(second, 1 - me[1], me[1])
        edge = jnp.logical_and(k >= models, k != joint)
        spot = jnp.where(second, k - joint - 2, jnp.where(k > joint, tiles, k - models))

        @pl.when(k == 1)
        def _():
            for copy in sides:
                copy.wait_send()
            for pair in strips:
                for copy in pair:
                    copy.start()

        @pl.when(k == inner - 1)
        def _():
            sides[0].wait_recv()

        @pl.when(k == joint)
        def _():
            sides[1].wait_recv()

        def landed(number, cut):
            there = pad.at[:, :, pl.ds(side * (nx + 2), 2), pl.ds(*cut), :]
            pltpu.make_async_copy(there, there, recv_sem.at[number]).wait()

        def strip(number):
            landed(2 + 2 * number + side, cuts[number])

        @pl.when(jnp.logical_and(edge, spot == 0))
        def _():
            strip(0)

            @pl.when(jnp.logical_not(outer))
            def _():
                hand(side).start()

            strip(1)

            @pl.when(outer)
            def _():
                hand(side).start()

            landed(first + 2 * side, before)

        for number in range(2, len(cuts)):
            @pl.when(jnp.logical_and(edge, spot == number))
            def _(number=number):
                strip(number)
                if number == len(cuts) - 1:
                    landed(first + 1 + 2 * side, behind)

        tile = jnp.where(edge, spot, jnp.where(k == joint, tiles, jnp.where(k == inner - 1, 0, k + 1)))
        start = jnp.where(edge, side * nx - 1, 1)
        count = jnp.where(edge, 1, jnp.where(jnp.logical_or(k < inner, k == joint), (nx - 2) // 2, 0))

        def strain_turn(row, carry):
            strains(start + 2 * row, tile)
            return carry
        lax.fori_loop(0, count, strain_turn, 0)

        model_tile = jnp.where(edge, spot - 1, jnp.where(k == joint, tiles - 1, k - inner + 1))
        block = jnp.where(edge, side * (nx - 2), 2)
        turns = jnp.where(edge, jnp.where(spot > 0, 1, 0), jnp.where(k < inner - 1, 0, (nx - 4) // 2))

        def model_turn(turn, carry):
            model(block + 2 * turn, model_tile)
            return carry
        lax.fori_loop(0, turns, model_turn, 0)
        return carry

    lax.fori_loop(0, joint + tiles + 3, step, 0)

    for number in range(2 * chunks):
        sent[0, number : number + 1, :] = jnp.sum(acc[number], axis=0, keepdims=True)
    for number in range(2 * chunks, ROWS):
        sent[0, number : number + 1, :] = jnp.zeros((1, LANES), jnp.float32)
    held = 2 * chunks

    def send(source, slot, number, other):
        pltpu.make_async_remote_copy(
            src_ref=sent.at[source, pl.ds(0, held)], dst_ref=got.at[slot, pl.ds(0, held)],
            send_sem=sum_send.at[0], recv_sem=sum_recv.at[number],
            device_id=other, device_id_type=MESH,
        ).start()

    def arrived(start, count, sem):
        there = got.at[pl.ds(start, count), pl.ds(0, held)]
        pltpu.make_async_copy(there, there, sem).wait()

    def added(terms):
        while len(terms) > 1:
            terms = [a + b for a, b in zip(terms[::2], terms[1::2])]
        return terms[0]

    line_at = 2 * members

    def to_outer(off):
        spot = shifted(in_plane, off)
        return (*spot[:4], nc - 1)

    def left():
        for copy in corners + [hand(0), hand(1)] + [strip for pair in strips for strip in pair]:
            copy.wait_send()

    @pl.when(jnp.logical_not(outer))
    def _():
        for off in plane_offs + [(0, 0, 0)]:
            send(0, plane_mine, 1, to_outer(off))
        left()
        arrived(0, members, sum_send.at[0])
        arrived(line_at, nz, sum_recv.at[2])

    @pl.when(outer)
    def _():
        for off in plane_offs:
            send(0, members + plane_mine, 1, shifted(in_plane, off))
        got[members + plane_mine] = sent[0]
        left()
        arrived(0, 2 * members - 1, sum_recv.at[1])
        whole = added([got[k] for k in range(2 * members)])
        sent[1] = whole
        for off in line_offs:
            send(1, line_at + me[0], 2, shifted(in_line, off))
        got[line_at + me[0]] = whole
        arrived(0, members - 1, sum_send.at[0])
        arrived(line_at, nz - 1, sum_recv.at[2])
        arrived(0, len(line_offs), sum_send.at[0])

    total = added([got[line_at + k] for k in range(nz)])

    for chunk in range(chunks):
        line = pl.ds(chunk * LANES, LANES)
        share = total[chunk : chunk + 1, :] * (1.0 / planes)
        below = total[chunks + chunk : chunks + chunk + 1, :] * (1.0 / planes) + 1e-06
        coefficient = share / below
        coef_out[0:1, line] = coefficient
        coef_out[1:2, line] = coefficient * gaps[3:4, line]


def finish(size, lm, mm, coef, eddy_out, lm_out, mm_out, coef_out, eddy, sem):
    copies = [
        pltpu.make_async_copy(lm, lm_out, sem.at[0]),
        pltpu.make_async_copy(mm, mm_out, sem.at[1]),
        pltpu.make_async_copy(coef.at[0], coef_out, sem.at[2]),
        pltpu.make_async_copy(eddy, eddy_out, sem.at[3]),
    ]
    for copy in copies[:3]:
        copy.start()
    eddy[...] = size[...] * coef[1:2, :].reshape(1, 1, coef.shape[1])
    copies[3].start()
    for copy in copies:
        copy.wait()


def solution(mesh):
    shape = (8, 2, 4, 2, 2)
    torus = Mesh(mesh.devices.reshape(shape), AXES)

    def per_device(velocity, y_gap):
        _, nx, depth, height = velocity.shape
        chunks, tiles = height // LANES, depth // ROWS
        cells = nx * lax.axis_size(GX) * depth * lax.axis_size(GZ)
        rims = 2 + 2 * len(CUTS) + 4
        ways = 2 * shape[1] * shape[2] * shape[3] + shape[0]
        grid = jax.ShapeDtypeStruct((nx, depth, height), jnp.float32)
        vmem = pl.BlockSpec(memory_space=pltpu.VMEM)
        hbm = pl.BlockSpec(memory_space=pltpu.HBM)
        size, lm, mm, coefficient = pl.pallas_call(
            lambda *refs: kernel(shape, cells, *refs),
            out_shape=(grid, grid, grid, jax.ShapeDtypeStruct((2, height), jnp.float32)),
            in_specs=[hbm, hbm],
            out_specs=(vmem, vmem, vmem, vmem),
            scratch_shapes=[
                pltpu.VMEM((3, chunks, nx + 4, depth + 16, LANES), jnp.float32),
                pltpu.VMEM((22, chunks, nx + 2, depth + 8, LANES), jnp.float32),
                pltpu.VMEM((height,), jnp.float32),
                pltpu.SMEM((height + 1,), jnp.float32),
                pltpu.VMEM((4, height), jnp.float32),
                pltpu.VMEM((2 * chunks, ROWS, LANES), jnp.float32),
                pltpu.VMEM((2, ROWS, LANES), jnp.float32),
                pltpu.VMEM((ways, ROWS, LANES), jnp.float32),
                pltpu.SemaphoreType.DMA((3 * chunks + 2,)),
                pltpu.SemaphoreType.DMA((rims,)),
                pltpu.SemaphoreType.DMA((rims,)),
                pltpu.SemaphoreType.DMA((1,)),
                pltpu.SemaphoreType.DMA((3,)),
            ],
            compiler_params=pltpu.CompilerParams(
                collective_id=0, has_side_effects=True, vmem_limit_bytes=40 * 1024 * 1024
            ),
            name="smagorinsky",
        )(pltpu.with_memory_space_constraint(velocity, pltpu.HBM), pltpu.with_memory_space_constraint(y_gap, pltpu.HBM))
        return pl.pallas_call(
            finish,
            out_shape=(grid, grid, grid, jax.ShapeDtypeStruct((height,), jnp.float32)),
            in_specs=[vmem] * 4,
            out_specs=[hbm] * 4,
            scratch_shapes=[pltpu.VMEM((nx, depth, height), jnp.float32), pltpu.SemaphoreType.DMA((4,))],
            compiler_params=pltpu.CompilerParams(vmem_limit_bytes=4 * 1024 * 1024),
            name="finish",
        )(size, lm, mm, coefficient)

    return jax.shard_map(
        per_device,
        mesh=torus,
        in_specs=(P(None, GX, GZ, None), P()),
        out_specs=(P(GX, GZ, None), P(GX, GZ, None), P(GX, GZ, None), P()),
        check_vma=False,
    )
```
